16 devices in a mesh: dp: 4 (over y, z, core), sp: 4 (over x).
Axes of the slice: x: 4, y: 2, z: 1, core: 2. Of those that a mesh axis runs over, the one named last changes fastest.
The devices are a block of a 4x4x8 slice.
Arguments:
- x: bfloat16 [16384, 4096], P(('dp', 'sp')), parts along dimension 0
- gain: bfloat16 [4096], replicated
- wq: bfloat16 [4096, 4096], P('sp')
- wk: bfloat16 [4096, 512], P('sp')
- wv: bfloat16 [4096, 512], P('sp')
- wo: bfloat16 [4096, 4096], P('sp')
Outputs:
- output: bfloat16 [16384, 4096], P(('dp', 'sp')), parts along dimension 0
There are 4 independent parts. The reference program is written for one: setup_inputs(seed, part) draws one part's arguments, and reference() takes and returns one part's arrays. A program takes and returns all parts, laid end to end along the dimension named above; an argument that names none is the same for every part.
All inputs are finite; a program needn't handle non-finite values.
Results may differ from the reference program's by a relative error of at most 0.012.
Values are sent between devices in bfloat16 or wider.
A program may use at most 768 MiB of HBM per device.

```python
import jax
import jax.numpy as jnp
from jax import lax

ROWS = 4096
D = 4096
HEADS = 32
KV_HEADS = 4
HEAD = 128
THETA = 10000


def setup_inputs(seed: int = 0, part: int = 0) -> dict:
    kx, kn, kq, kk, kv, ko = jax.random.split(jax.random.key(seed), 6)

    def weights(key, rows, columns):
        return jax.random.normal(key, (rows, columns), jnp.float32) * rows**-0.5

    drawn = {
        "x": jax.random.normal(jax.random.fold_in(kx, part), (ROWS, D), jnp.float32),
        "gain": 1 + 0.1 * jax.random.normal(kn, (D,), jnp.float32),
        "wq": 2 * weights(kq, D, HEADS * HEAD),
        "wk": 2 * weights(kk, D, KV_HEADS * HEAD),
        "wv": 4 * weights(kv, D, KV_HEADS * HEAD),
        "wo": weights(ko, HEADS * HEAD, D),
    }
    return {k: v.astype(jnp.bfloat16) for k, v in drawn.items()}


def normed(x, gain):
    wide = x.astype(jnp.float32)
    scale = lax.rsqrt(jnp.mean(wide * wide, -1, keepdims=True) + 1e-6)
    return (wide * scale * gain.astype(jnp.float32)).astype(jnp.bfloat16)


def turned(t, place, theta):
    half = t.shape[-1] // 2
    angle = place.astype(jnp.float32)[:, None] * theta ** (-jnp.arange(half, dtype=jnp.float32) / half)
    cos, sin = jnp.cos(angle)[:, None], jnp.sin(angle)[:, None]
    a, b = t[..., :half].astype(jnp.float32), t[..., half:].astype(jnp.float32)
    return jnp.concatenate([a * cos - b * sin, b * cos + a * sin], -1).astype(jnp.bfloat16)


def matmul(a, w):
    return jnp.dot(a, w, preferred_element_type=jnp.float32).astype(jnp.bfloat16)


def einsum(form, a, b):
    return jnp.einsum(form, a.astype(jnp.float32), b.astype(jnp.float32))


def attention(q, k, v):
    scores = einsum("tgsd,ugd->gstu", q, k) * q.shape[-1] ** -0.5
    token = jnp.arange(q.shape[0])
    scores = jnp.where(token[:, None] >= token, scores, -jnp.inf)
    weights = jax.nn.softmax(scores, -1).astype(jnp.bfloat16)
    return einsum("gstu,ugd->tgsd", weights, v).astype(jnp.bfloat16)


def reference(x, gain, wq, wk, wv, wo):
    a, place = normed(x, gain), jnp.arange(ROWS)
    q = turned(matmul(a, wq).reshape(ROWS, HEADS, HEAD), place, THETA).reshape(ROWS, KV_HEADS, -1, HEAD)
    k = turned(matmul(a, wk).reshape(ROWS, KV_HEADS, HEAD), place, THETA)
    v = matmul(a, wv).reshape(ROWS, KV_HEADS, HEAD)
    seen = attention(q, k, v).reshape(ROWS, HEADS * HEAD)
    return (x.astype(jnp.float32) + jnp.dot(seen, wo, preferred_element_type=jnp.float32)).astype(jnp.bfloat16)
```

```python
import functools

import jax
import jax.numpy as jnp
from jax import lax
from jax.experimental import pallas as pl
from jax.experimental.pallas import tpu as pltpu
from jax.sharding import PartitionSpec as P

NEG = -1e30
HIDDEN = 2 * NEG
LOG2E = 1.4426950408889634
HEAD = 128
THETA = 10000
CHUNK = 2 * HEAD
AHEAD = 3
MESH = pl.DeviceIdType.MESH


def _dot(a, b, ca, cb):
    return lax.dot_general(a, b, (((ca,), (cb,)), ((), ())), preferred_element_type=jnp.float32)


def _when(cond, f):
    if isinstance(cond, bool):
        if cond:
            f()
    else:
        pl.when(cond)(f)


class Place:
    def __init__(self, n):
        self.n = n
        self.me = lax.axis_index("sp")
        dp = lax.axis_index("dp")
        self.core, self.half = dp % 2, (dp // 2) % 2
        self.right, self.left, self.far = ((self.me + k) % n for k in (1, n - 1, 2))
        self.to_right, self.to_left = {"sp": self.right}, {"sp": self.left}
        self.to_core = {"dp": dp + 1 - 2 * self.core}
        self.to_pair = {"dp": dp + 2 - 4 * self.half}

    def greet(self, others):
        barrier = pltpu.get_barrier_semaphore()
        for other in others:
            pl.semaphore_signal(barrier, inc=1, device_id=other, device_id_type=MESH)
        pl.semaphore_wait(barrier, len(others))


def _remote(src, dst, sems, at, device):
    send, recv = sems
    return pltpu.make_async_remote_copy(
        src_ref=src, dst_ref=dst, send_sem=send.at[at], recv_sem=recv.at[at], device_id=device, device_id_type=MESH
    )


FROM_LEFT, FROM_RIGHT, ON_RIGHT, ON_LEFT, PAIR_L, PAIR_R, PAIR_F = range(7)


def _project(n, unique, rows, x_ref, gain_ref, wall_ref, cos_ref, sin_ref, out_ref, a_s, w_s, stage_s, send, recv, local, xsend, xrecv, xlocal,
             osem):
    p = Place(n)
    chunks, part = wall_ref.shape[0], wall_ref.shape[1]
    tokens = x_ref.shape[0]
    sems = (send, recv)
    common = part - 2 * unique
    reach = unique + common
    off_reach = p.half * unique
    off_mine = p.half * (part - unique)
    off_theirs = (1 - p.half) * (part - unique)
    unit = 16

    def at(j, owner, off, size):
        return w_s.at[j, pl.ds(pl.multiple_of(owner * part + off, unit), size), :]

    def hop(j, kind, owner, off, size, device):
        piece = at(j, owner, off, size)
        return _remote(piece, piece, sems, (j, kind), device)

    def own(j):
        src = wall_ref.at[j, pl.ds(pl.multiple_of(off_reach, unit), reach), :]
        dst = at(j, p.me, off_reach, reach)
        return [
            _remote(src, dst, sems, (j, FROM_LEFT), p.to_right),
            _remote(src, dst, sems, (j, FROM_RIGHT), p.to_left),
        ]

    def kept(j):
        return pltpu.make_async_copy(wall_ref.at[j], at(j, p.me, 0, part), local.at[j])

    def from_left(j):
        return hop(j, FROM_LEFT, p.left, off_reach, reach, p.to_right)

    def from_right(j):
        return hop(j, FROM_RIGHT, p.right, off_reach, reach, p.to_left)

    def passed(j):
        return [
            hop(j, ON_RIGHT, p.left, off_mine, unique, p.to_right),
            hop(j, PAIR_L, p.left, off_mine, unique, p.to_pair),
            hop(j, ON_LEFT, p.right, unique, common, p.to_left),
            hop(j, PAIR_R, p.right, off_mine, unique, p.to_pair),
        ]

    def last(j):
        return hop(j, PAIR_F, p.far, off_mine, unique, p.to_pair)

    swap = tokens // 4

    def x_local(t):
        r = pl.ds(t * swap, swap)
        return pltpu.make_async_copy(x_ref.at[r], a_s.at[0, r], xlocal.at[t])

    def x_swap(t):
        r = pl.ds(t * swap, swap)
        return _remote(x_ref.at[r], a_s.at[1, r], (xsend, xrecv), t, p.to_core)

    for t in range(4):
        x_local(t).start()
    p.greet([p.to_right, p.to_left, p.to_core, p.to_pair])
    for j in range(min(AHEAD, chunks)):
        for c in own(j):
            c.start()
        if j == 0:
            for t in range(4):
                x_swap(t).start()

    def keep(j, _):
        kept(j).start()

    lax.fori_loop(0, chunks, keep, None)

    def normalize(g, first, count):
        def body(b, _):
            r = pl.ds(pl.multiple_of(b * 32, 32), 32)
            wide = a_s[g, r, :].astype(jnp.float32)
            scale = lax.rsqrt(jnp.mean(wide * wide, -1, keepdims=True) + 1e-6)
            a_s[g, r, :] = (a_s[g, r, :].astype(jnp.float32) * scale * gain_ref[...].astype(jnp.float32)).astype(jnp.bfloat16)

        lax.fori_loop(first // 32, (first + count) // 32, body, None)

    for t in range(4):
        x_local(t).wait()
        normalize(0, t * swap, swap)
    for t in range(4):
        x_swap(t).wait_recv()
        normalize(1, t * swap, swap)

    def compute(j):
        slot = j % 2
        plain = j == 1

        def body(b, _):
            g, m = b // (tokens // rows), b % (tokens // rows)
            r = pl.ds(pl.multiple_of(m * rows, rows), rows)
            t = _dot(a_s[g, r, :], w_s[j], 1, 0).astype(jnp.bfloat16)
            cos, sin = cos_ref[r, :], sin_ref[r, :]
            for h in range(2):
                u = t[:, h * HEAD : (h + 1) * HEAD].astype(jnp.float32)
                v = u * cos + pltpu.roll(u, HEAD // 2, 1) * sin
                stage_s[slot, g, h, r, :] = jnp.where(plain, u, v).astype(jnp.bfloat16)

        lax.fori_loop(0, 2 * (tokens // rows), body, None)

    def out(j):
        return pltpu.make_async_copy(stage_s.at[j % 2], out_ref.at[j], osem.at[j % 2])

    def turn(j, _):
        @pl.when(j < chunks)
        def _():
            from_left(j).wait_recv()
            go = passed(j)
            go[0].start()
            go[1].start()
            from_right(j).wait_recv()
            go[2].start()
            go[3].start()

        @pl.when(j + AHEAD < chunks)
        def _():
            for c in own(j + AHEAD):
                c.start()

        @pl.when((j >= 1) & (j <= chunks))
        def _():
            i = j - 1
            hop(i, ON_RIGHT, p.far, off_mine, unique, p.to_right).wait_recv()
            last(i).start()

        @pl.when(j >= 2)
        def _():
            i = j - 2
            kept(i).wait()
            hop(i, ON_LEFT, p.far, unique, common, p.to_left).wait_recv()
            hop(i, PAIR_L, p.left, off_theirs, unique, p.to_pair).wait_recv()
            hop(i, PAIR_R, p.right, off_theirs, unique, p.to_pair).wait_recv()
            hop(i, PAIR_F, p.far, off_theirs, unique, p.to_pair).wait_recv()

            @pl.when(i >= 2)
            def _():
                out(i - 2).wait()

            compute(i)
            out(i).start()

    lax.fori_loop(0, chunks + 2, turn, None)

    out(chunks - 2).wait()
    out(chunks - 1).wait()
    for t in range(4):
        x_swap(t).wait_send()

    def drain(j, _):
        for c in [*own(j), *passed(j), last(j)]:
            c.wait_send()

    lax.fori_loop(0, chunks, drain, None)


def project(n, x, gain, wall, cos, sin):
    tokens, width = x.shape
    chunks, part, _ = wall.shape
    unique = part * 11 // 32 // 16 * 16
    rows = min(512, tokens)
    anywhere, vmem = pl.BlockSpec(memory_space=pl.ANY), pl.BlockSpec(memory_space=pltpu.VMEM)
    return pl.pallas_call(
        functools.partial(_project, n, unique, rows),
        out_shape=jax.ShapeDtypeStruct((chunks, 2, 2, tokens, HEAD), jnp.bfloat16),
        in_specs=[anywhere, vmem, anywhere, vmem, vmem],
        out_specs=anywhere,
        scratch_shapes=[
            pltpu.VMEM((2, tokens, width), jnp.bfloat16),
            pltpu.VMEM((chunks, width, CHUNK), jnp.bfloat16),
            pltpu.VMEM((2, 2, 2, tokens, HEAD), jnp.bfloat16),
            pltpu.SemaphoreType.DMA((chunks, 7)),
            pltpu.SemaphoreType.DMA((chunks, 7)),
            pltpu.SemaphoreType.DMA((chunks,)),
            pltpu.SemaphoreType.DMA((4,)),
            pltpu.SemaphoreType.DMA((4,)),
            pltpu.SemaphoreType.DMA((4,)),
            pltpu.SemaphoreType.DMA((2,)),
        ],
        compiler_params=pltpu.CompilerParams(collective_id=0, has_side_effects=True, vmem_limit_bytes=60 * 2**20),
        cost_estimate=pl.CostEstimate(flops=4 * tokens * width * chunks * CHUNK, transcendentals=0, bytes_accessed=2**26),
        name="project",
    )(x, gain, wall, cos, sin)


A_LEFT, A_RIGHT, F_LEFT, F_RIGHT, Y_L, Y_R, Y_F, D_L, D_R, D_F, E_L, E_R, E_F = range(13)
KINDS = 13


def _attend(n, bq, cut, e, kvq_ref, wo_ref, seen_ref, all_ref, q_s, kv_s, top_s, mix_s, stage_s, send, recv, ksend, krecv, rsend, rrecv, lsem, ssem,
            wsem):
    p = Place(n)
    part = wo_ref.shape[0]
    qchunks, tokens = q_s.shape[0], q_s.shape[3]
    kvh = kv_s.shape[3]
    strips = qchunks // kvh
    wide = 2 * bq
    steps = tokens // bq
    width = qchunks * CHUNK
    cw = width // cut
    half = part // 2
    off, other = p.half * half, (1 - p.half) * half
    sems = (send, recv)

    def block_of(owner, o, size, core, m):
        return all_ref.at[pl.ds(pl.multiple_of(owner * part + o, 16), size), pl.ds(pl.multiple_of(core * width + m * cw, 128), cw)]

    def hop(m, kind, owner, o, size, device, core=None):
        piece = block_of(owner, o, size, p.core if core is None else core, m)
        return _remote(piece, piece, sems, (m, kind), device)

    def own(m):
        src = wo_ref.at[pl.ds(pl.multiple_of(off, 16), half), pl.ds(pl.multiple_of(p.core * width + m * cw, 128), cw)]
        dst = block_of(p.me, off, half, p.core, m)
        return [_remote(src, dst, sems, (m, A_LEFT), p.to_right), _remote(src, dst, sems, (m, A_RIGHT), p.to_left)]

    quarter = half // 2

    def first(m):
        return [
            hop(m, F_LEFT, p.left, off, quarter, p.to_right),
            hop(m, Y_L, p.left, off, half, p.to_pair),
            hop(m, D_L, p.left, off, half, p.to_core),
            hop(m, F_RIGHT, p.right, off + quarter, quarter, p.to_left),
            hop(m, Y_R, p.right, off, half, p.to_pair),
            hop(m, D_R, p.right, off, half, p.to_core),
        ]

    def second(m):
        return [hop(m, Y_F, p.far, off, half, p.to_pair), hop(m, D_F, p.far, off, half, p.to_core)]

    def third(m):
        return [
            hop(m, E_L, p.left, other, half, p.to_core),
            hop(m, E_R, p.right, other, half, p.to_core),
            hop(m, E_F, p.far, other, half, p.to_core),
        ]

    def go_own(m):
        for c in own(m):
            c.start()

    def go_first(m):
        hop(m, A_LEFT, p.left, off, half, p.to_right).wait_recv()
        go = first(m)
        for c in go[:3]:
            c.start()
        hop(m, A_RIGHT, p.right, off, half, p.to_left).wait_recv()
        for c in go[3:]:
            c.start()

    def go_second(m):
        hop(m, F_LEFT, p.far, off, quarter, p.to_right).wait_recv()
        hop(m, F_RIGHT, p.far, off + quarter, quarter, p.to_left).wait_recv()
        for c in second(m):
            c.start()

    def go_third(m):
        got = [hop(m, Y_L, p.left, other, half, p.to_pair), hop(m, Y_R, p.right, other, half, p.to_pair), hop(m, Y_F, p.far, other, half, p.to_pair)]
        for c, d in zip(got, third(m)):
            c.wait_recv()
            d.start()

    def finish(m):
        core = 1 - p.core
        for kind, owner, o in ((D_L, p.left, off), (D_R, p.right, off), (D_F, p.far, off), (E_L, p.left, other), (E_R, p.right, other), (E_F, p.far, other)):
            hop(m, kind, owner, o, half, p.to_core, core).wait_recv()
        for c in [*own(m), *first(m), *second(m), *third(m)]:
            c.wait_send()

    def keys(r, g):
        return _remote(kvq_ref.at[0:2, g], kv_s.at[r, :, g], (ksend, krecv), (r, g), {"sp": (p.me + r) % n})

    def send_keys(r, g):
        @pl.when(p.me + r < n)
        def _():
            keys(r, g).start()

    def here(g):
        return [
            pltpu.make_async_copy(kvq_ref.at[0:2, g], kv_s.at[0, :, g], lsem.at[g, 0]),
            pltpu.make_async_copy(kvq_ref.at[2:, g], q_s.at[:, g], lsem.at[g, 1]),
        ]

    mine = pltpu.make_async_copy(wo_ref, all_ref.at[pl.ds(pl.multiple_of(p.me * part, 16), part)], wsem)

    for g in range(2):
        for c in here(g):
            c.start()
    p.greet([{"sp": (p.me + k) % n} for k in range(1, n)] + [p.to_core, p.to_pair])

    ones = jnp.ones((8, 2 * bq), jnp.bfloat16)
    pieces = [(i, s) for i in range(kvh) for s in range(strips)]

    def block(st, g, iq, r, key0, bk, diagonal):
        rows, span = pl.ds(pl.multiple_of(iq * bq, bq), bq), pl.ds(pl.multiple_of(key0, bq), bk)
        scores = [
            _dot(kv_s[r, 0, g, i, span, :], q_s[i * strips + s, g, :, rows, :].reshape(wide, HEAD), 1, 1) for i, s in pieces
        ]
        weights, keeps = [], []
        if diagonal:
            ok = lax.rem(lax.broadcasted_iota(jnp.int32, (bk, wide), 1), bq) >= lax.broadcasted_iota(jnp.int32, (bk, wide), 0)
        for (i, s), x in zip(pieces, scores):
            cols = slice(s * wide, (s + 1) * wide)
            if diagonal:
                x = jnp.where(ok, x, HIDDEN)
                top = x.max(axis=0, keepdims=True)
                keeps.append(None)
            else:
                old = top_s[st, i : i + 1, cols]
                top = jnp.maximum(old, x.max(axis=0, keepdims=True))
                keeps.append(jnp.exp2((old - top) * e))
            top_s[st, i : i + 1, cols] = top
            weights.append(jnp.exp2((x - top) * e).astype(jnp.bfloat16))
        for (i, s), w, keep in zip(pieces, weights, keeps):
            cols = slice(s * wide, (s + 1) * wide)
            values = jnp.concatenate([kv_s[r, 1, g, i, span, :].T, ones[:, :bk]], axis=0)
            new = _dot(values, w, 1, 0)
            mix_s[st, i, :, cols] = new if keep is None else mix_s[st, i, :, cols] * keep + new

    phases = [(0, 0), (0, 1)] + [(r, g) for r in (1, 3, 2) for g in range(2)][: 2 * (n - 1)]

    def phase(ph, _):
        g = ph % 2
        kk = ph // 2
        r = jnp.where(kk == 2, n - 1, jnp.where(kk == 3, 2, kk))

        for k in range(len(events)):
            @pl.when(ph == k)
            def _(k=k):
                for f, a in events[k]:
                    f(*a)

        @pl.when(ph < 2)
        def _():
            for c in here(g):
                c.wait()

            def step(iq, _):
                st = g * steps + iq
                block(st, g, iq, 0, iq * bq, bq, True)
                lax.fori_loop(0, iq, lambda b, _: block(st, g, iq, 0, b * bq, bq, False), None)

            lax.fori_loop(0, steps, step, None)

        @pl.when((ph >= 2) & (p.me >= r))
        def _():
            keys(r, g).wait_recv()

            def step(iq, _):
                st = g * steps + iq
                lax.fori_loop(0, tokens // (2 * bq), lambda b, _: block(st, g, iq, r, b * 2 * bq, 2 * bq, False), None)

            lax.fori_loop(0, steps, step, None)

    E = [[] for _ in range(len(phases))]
    E[0] = [(go_own, (0,)), (send_keys, (1, 0)), (send_keys, (3, 0)), (send_keys, (1, 1)), (send_keys, (3, 1)), (go_own, (1,)), (mine.start, ())]
    E[1] = [(go_first, (0,))]
    E[2] = [(go_second, (0,)), (send_keys, (2, 0)), (go_own, (2,))]
    E[3] = [(go_first, (1,)), (send_keys, (2, 1)), (go_own, (3,))]
    E[4] = [(go_second, (1,)), (go_first, (2,)), (go_third, (0,))]
    E[5] = [(go_second, (2,)), (go_first, (3,))]
    E[6] = [(go_third, (1,)), (go_second, (3,))]
    E[7] = [(go_third, (2,))]
    events = E
    lax.fori_loop(0, len(phases), phase, None)

    def result(g, iq):
        rows, cols = pl.ds(pl.multiple_of(iq * bq, bq), bq), pl.ds(pl.multiple_of(p.core * width, 128), width)
        return stage_s.at[(g * steps + iq) % 2], seen_ref.at[rows, cols]

    def swapped(iq):
        return _remote(*result(1, iq), (rsend, rrecv), iq, p.to_core)

    def stored(iq):
        return pltpu.make_async_copy(*result(0, iq), ssem.at[iq])

    def close(g, iq):
        st, slot = g * steps + iq, (g * steps + iq) % 2
        for i in range(kvh):
            for h in range(2 * strips):
                cols = slice(h * bq, (h + 1) * bq)
                u = mix_s[st, i, :HEAD, cols] * (1 / mix_s[st, i, HEAD : HEAD + 1, cols])
                at = (i * 2 * strips + h) * HEAD
                stage_s[slot, :, at : at + HEAD] = u.T.astype(jnp.bfloat16)

    def close_other(iq, _):
        @pl.when(iq >= 2)
        def _():
            swapped(iq - 2).wait_send()

        close(1, iq)
        swapped(iq).start()

    def close_own(iq, _):
        @pl.when(iq >= 2)
        def _():
            stored(iq - 2).wait()

        close(0, iq)
        stored(iq).start()

    lax.fori_loop(0, steps, close_other, None)
    for iq in (steps - 2, steps - 1):
        swapped(iq).wait_send()
    lax.fori_loop(0, steps, close_own, None)
    go_third(3)
    for iq in (steps - 2, steps - 1):
        stored(iq).wait()
    rows = lambda iq: seen_ref.at[pl.ds(iq * bq, bq), pl.ds(pl.multiple_of((1 - p.core) * width, 128), width)]
    for iq in range(steps):
        _remote(stage_s.at[0], rows(iq), (rsend, rrecv), iq, p.to_core).wait_recv()
    for m in range(cut):
        finish(m)
    for r in range(1, n):
        for g in range(2):
            @pl.when(p.me + r < n)
            def _(r=r, g=g):
                keys(r, g).wait_send()

    mine.wait()


def attend(n, kvq, wo):
    chunks, _, kvh, tokens, _ = kvq.shape
    part, width = wo.shape
    q = chunks - 2
    bq = tokens // 4
    steps = 4
    cut = 4
    cols = (q // kvh) * 2 * bq
    anywhere = pl.BlockSpec(memory_space=pl.ANY)
    scores = 2 * 2 * q * tokens * tokens * n
    return pl.pallas_call(
        functools.partial(_attend, n, bq, cut, HEAD**-0.5 * LOG2E),
        out_shape=[jax.ShapeDtypeStruct((tokens, width), jnp.bfloat16), jax.ShapeDtypeStruct((n * part, width), jnp.bfloat16)],
        in_specs=[anywhere, anywhere],
        out_specs=[anywhere, anywhere],
        scratch_shapes=[
            pltpu.VMEM((q, 2, 2, tokens, HEAD), jnp.bfloat16),
            pltpu.VMEM((n, 2, 2, kvh, tokens, HEAD), jnp.bfloat16),
            pltpu.VMEM((2 * steps, kvh, cols), jnp.float32),
            pltpu.VMEM((2 * steps, kvh, HEAD + 8, cols), jnp.float32),
            pltpu.VMEM((2, bq, q * CHUNK), jnp.bfloat16),
            pltpu.SemaphoreType.DMA((cut, KINDS)),
            pltpu.SemaphoreType.DMA((cut, KINDS)),
            pltpu.SemaphoreType.DMA((n, 2)),
            pltpu.SemaphoreType.DMA((n, 2)),
            pltpu.SemaphoreType.DMA((steps,)),
            pltpu.SemaphoreType.DMA((steps,)),
            pltpu.SemaphoreType.DMA((2, 2)),
            pltpu.SemaphoreType.DMA((steps,)),
            pltpu.SemaphoreType.DMA,
        ],
        compiler_params=pltpu.CompilerParams(collective_id=1, has_side_effects=True, vmem_limit_bytes=62 * 2**20),
        cost_estimate=pl.CostEstimate(flops=4 * HEAD * scores // 4, transcendentals=scores // 4, bytes_accessed=2**26),
        name="attend",
    )(kvq, wo)


def solution(mesh):
    n = mesh.shape["sp"]

    def step(x, gain, wq, wk, wv, wo):
        tokens = x.shape[0]
        core = lax.axis_index("dp") % 2

        def mine(w):
            w = lax.dynamic_slice_in_dim(w, core * (w.shape[1] // 2), w.shape[1] // 2, axis=1)
            return w.reshape(w.shape[0], -1, CHUNK).transpose(1, 0, 2)

        wall = jnp.concatenate([mine(w) for w in (wk, wv, wq)], axis=0)
        place = lax.axis_index("sp") * tokens + jnp.arange(tokens)
        half = HEAD // 2
        angle = place.astype(jnp.float32)[:, None] * THETA ** (-jnp.arange(half, dtype=jnp.float32) / half)
        cos, sin = jnp.cos(angle), jnp.sin(angle)
        cos, sin = jnp.concatenate([cos, cos], 1), jnp.concatenate([-sin, sin], 1)
        kvq = project(n, x, gain[None], wall, cos, sin)
        seen, wo = attend(n, kvq, wo)
        y = jnp.dot(seen, wo, preferred_element_type=jnp.float32)
        return (x.astype(jnp.float32) + y).astype(jnp.bfloat16)

    tokens, whole = P(("dp", "sp"), None), P("sp", None)
    return jax.shard_map(
        step,
        mesh=mesh,
        in_specs=(tokens, P(None), whole, whole, whole, whole),
        out_specs=tokens,
        check_vma=False,
    )
```

```python
import functools

import jax
import jax.numpy as jnp
from jax import lax
from jax.experimental import pallas as pl
from jax.experimental.pallas import tpu as pltpu
from jax.sharding import PartitionSpec as P

NEG = -1e30
HIDDEN = 2 * NEG
LOG2E = 1.4426950408889634
HEAD = 128
THETA = 10000
CHUNK = 2 * HEAD
AHEAD = 3
MESH = pl.DeviceIdType.MESH


def _dot(a, b, ca, cb):
    return lax.dot_general(a, b, (((ca,), (cb,)), ((), ())), preferred_element_type=jnp.float32)


def _when(cond, f):
    if isinstance(cond, bool):
        if cond:
            f()
    else:
        pl.when(cond)(f)


class Place:
    def __init__(self, n):
        self.n = n
        self.me = lax.axis_index("sp")
        dp = lax.axis_index("dp")
        self.core, self.half = dp % 2, (dp // 2) % 2
        self.right, self.left, self.far = ((self.me + k) % n for k in (1, n - 1, 2))
        self.to_right, self.to_left = {"sp": self.right}, {"sp": self.left}
        self.to_core = {"dp": dp + 1 - 2 * self.core}
        self.to_pair = {"dp": dp + 2 - 4 * self.half}

    def greet(self, others):
        barrier = pltpu.get_barrier_semaphore()
        for other in others:
            pl.semaphore_signal(barrier, inc=1, device_id=other, device_id_type=MESH)
        pl.semaphore_wait(barrier, len(others))


def _remote(src, dst, sems, at, device):
    send, recv = sems
    return pltpu.make_async_remote_copy(
        src_ref=src, dst_ref=dst, send_sem=send.at[at], recv_sem=recv.at[at], device_id=device, device_id_type=MESH
    )


FROM_LEFT, FROM_RIGHT, ON_RIGHT, ON_LEFT, PAIR_L, PAIR_R, PAIR_F = range(7)


def _project(n, unique, rows, x_ref, gain_ref, wk_ref, wv_ref, wq_ref, cos_ref, sin_ref, out_ref, a_s, w_s, stage_s, cos_s, sin_s, gain_s, send, recv,
             local, xsend, xrecv, xlocal, osem):
    p = Place(n)
    chunks, part = w_s.shape[0], wq_ref.shape[0]
    tokens = x_ref.shape[0]
    sems = (send, recv)
    common = part - 2 * unique
    reach = unique + common
    off_reach = p.half * unique
    off_mine = p.half * (part - unique)
    off_theirs = (1 - p.half) * (part - unique)
    unit = 16

    def at(j, owner, off, size):
        return w_s.at[j, pl.ds(pl.multiple_of(owner * part + off, unit), size), :]

    def hop(j, kind, owner, off, size, device):
        piece = at(j, owner, off, size)
        return _remote(piece, piece, sems, (j, kind), device)

    def source(j, rows):
        w, first = (wk_ref, 0) if isinstance(j, int) and j == 0 else (wv_ref, 0) if isinstance(j, int) and j == 1 else (wq_ref, jnp.maximum(j - 2, 0))
        return w.at[rows, pl.ds(pl.multiple_of(p.core * (w.shape[1] // 2) + first * CHUNK, HEAD), CHUNK)]

    def own(j):
        src = source(j, pl.ds(pl.multiple_of(off_reach, unit), reach))
        dst = at(j, p.me, off_reach, reach)
        return [
            _remote(src, dst, sems, (j, FROM_LEFT), p.to_right),
            _remote(src, dst, sems, (j, FROM_RIGHT), p.to_left),
        ]

    def kept(j):
        return pltpu.make_async_copy(source(j, pl.ds(0, part)), at(j, p.me, 0, part), local.at[j])

    def from_left(j):
        return hop(j, FROM_LEFT, p.left, off_reach, reach, p.to_right)

    def from_right(j):
        return hop(j, FROM_RIGHT, p.right, off_reach, reach, p.to_left)

    def passed(j):
        return [
            hop(j, ON_RIGHT, p.left, off_mine, unique, p.to_right),
            hop(j, PAIR_L, p.left, off_mine, unique, p.to_pair),
            hop(j, ON_LEFT, p.right, unique, common, p.to_left),
            hop(j, PAIR_R, p.right, off_mine, unique, p.to_pair),
        ]

    def last(j):
        return hop(j, PAIR_F, p.far, off_mine, unique, p.to_pair)

    swap = tokens // 4

    def x_local(t):
        r = pl.ds(t * swap, swap)
        return pltpu.make_async_copy(x_ref.at[r], a_s.at[0, r], xlocal.at[t])

    def x_swap(t):
        r = pl.ds(t * swap, swap)
        return _remote(x_ref.at[r], a_s.at[1, r], (xsend, xrecv), t, p.to_core)

    for t in range(4):
        x_local(t).start()
    p.greet([p.to_right, p.to_left, p.to_core, p.to_pair])
    for j in range(min(AHEAD, chunks)):
        for c in own(j):
            c.start()
        if j == 0:
            for t in range(4):
                x_swap(t).start()

    def keep(j, _):
        kept(j).start()

    keep(0, None)
    keep(1, None)
    lax.fori_loop(2, chunks, keep, None)

    cos_s[...] = jnp.concatenate([cos_ref[...], cos_ref[...]], axis=1)
    sin_s[...] = jnp.concatenate([-sin_ref[...], sin_ref[...]], axis=1)
    for i in range(gain_ref.shape[0]):
        gain_s[:, i * HEAD : (i + 1) * HEAD] = gain_ref[i : i + 1, :].astype(jnp.float32)

    def normalize(g, first, count):
        def body(b, _):
            r = pl.ds(pl.multiple_of(b * 32, 32), 32)
            wide = a_s[g, r, :].astype(jnp.float32)
            scale = lax.rsqrt(jnp.mean(wide * wide, -1, keepdims=True) + 1e-6)
            a_s[g, r, :] = (a_s[g, r, :].astype(jnp.float32) * scale * gain_s[...]).astype(jnp.bfloat16)

        lax.fori_loop(first // 32, (first + count) // 32, body, None)

    for t in range(4):
        x_local(t).wait()
        normalize(0, t * swap, swap)
    for t in range(4):
        x_swap(t).wait_recv()
        normalize(1, t * swap, swap)

    def compute(j):
        slot = j % 2
        plain = j == 1

        def body(b, _):
            g, m = b // (tokens // rows), b % (tokens // rows)
            r = pl.ds(pl.multiple_of(m * rows, rows), rows)
            t = _dot(a_s[g, r, :], w_s[j], 1, 0).astype(jnp.bfloat16)
            cos, sin = cos_s[r, :], sin_s[r, :]
            for h in range(2):
                u = t[:, h * HEAD : (h + 1) * HEAD].astype(jnp.float32)
                v = u * cos + pltpu.roll(u, HEAD // 2, 1) * sin
                stage_s[slot, g, h, r, :] = jnp.where(plain, u, v).astype(jnp.bfloat16)

        lax.fori_loop(0, 2 * (tokens // rows), body, None)

    def out(j):
        return pltpu.make_async_copy(stage_s.at[j % 2], out_ref.at[j], osem.at[j % 2])

    def turn(j, _):
        @pl.when(j < chunks)
        def _():
            from_left(j).wait_recv()
            go = passed(j)
            go[0].start()
            go[1].start()
            from_right(j).wait_recv()
            go[2].start()
            go[3].start()

        @pl.when(j + AHEAD < chunks)
        def _():
            for c in own(j + AHEAD):
                c.start()

        @pl.when((j >= 1) & (j <= chunks))
        def _():
            i = j - 1
            hop(i, ON_RIGHT, p.far, off_mine, unique, p.to_right).wait_recv()
            last(i).start()

        @pl.when(j >= 2)
        def _():
            i = j - 2
            kept(i).wait()
            hop(i, ON_LEFT, p.far, unique, common, p.to_left).wait_recv()
            hop(i, PAIR_L, p.left, off_theirs, unique, p.to_pair).wait_recv()
            hop(i, PAIR_R, p.right, off_theirs, unique, p.to_pair).wait_recv()
            hop(i, PAIR_F, p.far, off_theirs, unique, p.to_pair).wait_recv()

            @pl.when(i >= 2)
            def _():
                out(i - 2).wait()

            compute(i)
            out(i).start()

    lax.fori_loop(0, chunks + 2, turn, None)

    out(chunks - 2).wait()
    out(chunks - 1).wait()
    for t in range(4):
        x_swap(t).wait_send()

    def drain(j, _):
        for c in [*own(j), *passed(j), last(j)]:
            c.wait_send()

    lax.fori_loop(0, chunks, drain, None)


def project(n, x, gain, wk, wv, wq, cos, sin):
    tokens, width = x.shape
    part = wq.shape[0]
    chunks = (wk.shape[1] + wv.shape[1] + wq.shape[1]) // (2 * CHUNK)
    unique = part * 11 // 32 // 16 * 16
    rows = min(512, tokens)
    anywhere, vmem = pl.BlockSpec(memory_space=pl.ANY), pl.BlockSpec(memory_space=pltpu.VMEM)
    return pl.pallas_call(
        functools.partial(_project, n, unique, rows),
        out_shape=jax.ShapeDtypeStruct((chunks, 2, 2, tokens, HEAD), jnp.bfloat16),
        in_specs=[anywhere, vmem, anywhere, anywhere, anywhere, vmem, vmem],
        out_specs=anywhere,
        scratch_shapes=[
            pltpu.VMEM((2, tokens, width), jnp.bfloat16),
            pltpu.VMEM((chunks, width, CHUNK), jnp.bfloat16),
            pltpu.VMEM((2, 2, 2, tokens, HEAD), jnp.bfloat16),
            pltpu.VMEM((tokens, HEAD), jnp.float32),
            pltpu.VMEM((tokens, HEAD), jnp.float32),
            pltpu.VMEM((1, width), jnp.float32),
            pltpu.SemaphoreType.DMA((chunks, 7)),
            pltpu.SemaphoreType.DMA((chunks, 7)),
            pltpu.SemaphoreType.DMA((chunks,)),
            pltpu.SemaphoreType.DMA((4,)),
            pltpu.SemaphoreType.DMA((4,)),
            pltpu.SemaphoreType.DMA((4,)),
            pltpu.SemaphoreType.DMA((2,)),
        ],
        compiler_params=pltpu.CompilerParams(collective_id=0, has_side_effects=True, vmem_limit_bytes=60 * 2**20),
        cost_estimate=pl.CostEstimate(flops=4 * tokens * width * chunks * CHUNK, transcendentals=0, bytes_accessed=2**26),
        name="project",
    )(x, gain.reshape(-1, HEAD), wk, wv, wq, cos, sin)


A_LEFT, A_RIGHT, F_LEFT, F_RIGHT, Y_L, Y_R, Y_F, D_L, D_R, D_F, E_L, E_R, E_F = range(13)
KINDS = 13


def _attend(n, bq, cut, unique, e, kvq_ref, wo_ref, seen_ref, all_ref, q_s, kv_s, top_s, mix_s, stage_s, wo_s, send, recv, ksend, krecv, rsend, rrecv, lsem, ssem,
            wsem):
    p = Place(n)
    part = wo_ref.shape[0]
    qchunks, tokens = q_s.shape[0], q_s.shape[3]
    kvh = kv_s.shape[3]
    strips = qchunks // kvh
    wide = 2 * bq
    steps = tokens // bq
    width = qchunks * CHUNK
    cw = width // cut
    reach = part - unique
    off, mid = p.half * unique, reach // 2
    off_mine, other = p.half * reach, (1 - p.half) * reach
    sems = (send, recv)

    def block_of(owner, o, size, core, m):
        return all_ref.at[pl.ds(pl.multiple_of(owner * part + o, 16), size), pl.ds(pl.multiple_of(core * width + m * cw, 128), cw)]

    def hop(m, kind, owner, o, size, device, core=None):
        piece = block_of(owner, o, size, p.core if core is None else core, m)
        return _remote(piece, piece, sems, (m, kind), device)

    def own(m):
        src = wo_ref.at[pl.ds(pl.multiple_of(off, 16), reach), pl.ds(pl.multiple_of(p.core * width + m * cw, 128), cw)]
        dst = block_of(p.me, off, reach, p.core, m)
        return [_remote(src, dst, sems, (m, A_LEFT), p.to_right), _remote(src, dst, sems, (m, A_RIGHT), p.to_left)]

    def first(m):
        return [
            hop(m, F_LEFT, p.left, off, mid, p.to_right),
            hop(m, Y_L, p.left, off_mine, unique, p.to_pair),
            hop(m, D_L, p.left, off, reach, p.to_core),
            hop(m, F_RIGHT, p.right, off + mid, reach - mid, p.to_left),
            hop(m, Y_R, p.right, off_mine, unique, p.to_pair),
            hop(m, D_R, p.right, off, reach, p.to_core),
        ]

    def second(m):
        return [hop(m, Y_F, p.far, off_mine, unique, p.to_pair), hop(m, D_F, p.far, off, reach, p.to_core)]

    def third(m):
        return [
            hop(m, E_L, p.left, other, unique, p.to_core),
            hop(m, E_R, p.right, other, unique, p.to_core),
            hop(m, E_F, p.far, other, unique, p.to_core),
        ]

    def go_own(m):
        for c in own(m):
            c.start()

    def go_first(m):
        hop(m, A_LEFT, p.left, off, reach, p.to_right).wait_recv()
        go = first(m)
        for c in go[:3]:
            c.start()
        hop(m, A_RIGHT, p.right, off, reach, p.to_left).wait_recv()
        for c in go[3:]:
            c.start()

    def go_second(m):
        hop(m, F_LEFT, p.far, off, mid, p.to_right).wait_recv()
        hop(m, F_RIGHT, p.far, off + mid, reach - mid, p.to_left).wait_recv()
        for c in second(m):
            c.start()

    def go_third(m):
        got = [hop(m, Y_L, p.left, other, unique, p.to_pair), hop(m, Y_R, p.right, other, unique, p.to_pair), hop(m, Y_F, p.far, other, unique, p.to_pair)]
        for c, d in zip(got, third(m)):
            c.wait_recv()
            d.start()

    def finish(m):
        core = 1 - p.core
        for kinds, o, size in (((D_L, D_R, D_F), off, reach), ((E_L, E_R, E_F), other, unique)):
            for kind, owner in zip(kinds, (p.left, p.right, p.far)):
                hop(m, kind, owner, o, size, p.to_core, core).wait_recv()
        for c in [*own(m), *first(m), *second(m), *third(m)]:
            c.wait_send()

    def keys(r, g, source=None, device=None, kind=None):
        src = kvq_ref.at[0:2, g] if source is None else kv_s.at[source, :, g]
        return pltpu.make_async_remote_copy(
            src_ref=src, dst_ref=kv_s.at[r, :, g], send_sem=ksend.at[r if kind is None else kind, g], recv_sem=krecv.at[r, g],
            device_id=p.to_right if device is None else device, device_id_type=MESH,
        )

    def key_sends(g):
        routes = [(p.me < n - 1, (1, g)), (p.me == 0, (n - 1, g, None, p.to_left))]
        if g == 1:
            routes += [(p.me == 1, (1, g, None, p.to_left, 2)), (p.me == 0, (2, g, 1, p.to_left, 2))]
        else:
            routes += [(p.me == 2, (2, g, 1, p.to_right, 2))]
        return routes + [(p.me == n - 1, (2, g, n - 1, p.to_left, 2))]

    def send_keys(*which):
        for g, at in which:
            who, copy = key_sends(g)[at]
            pl.when(who)(lambda: keys(*copy).start())

    def pass_on():
        @pl.when(p.me == 0)
        def _():
            keys(1, 1).wait_recv()
            keys(2, 1, 1, p.to_left, 2).start()

    strip = part // 8

    def take(t):
        return pltpu.make_async_copy(wo_ref.at[pl.ds(t * strip, strip)], wo_s.at[t % 2], wsem.at[0, t % 2])

    def put(t):
        return pltpu.make_async_copy(
            wo_s.at[t % 2], all_ref.at[pl.ds(pl.multiple_of(p.me * part + t * strip, 16), strip)], wsem.at[1, t % 2]
        )

    def keep_own(t):
        if t >= 2:
            put(t - 2).wait()
        if t < 8:
            take(t).start()
        if 1 <= t <= 8:
            take(t - 1).wait()
            put(t - 1).start()

    def here(g):
        return [
            pltpu.make_async_copy(kvq_ref.at[0:2, g], kv_s.at[0, :, g], lsem.at[g, 0]),
            pltpu.make_async_copy(kvq_ref.at[2:, g], q_s.at[:, g], lsem.at[g, 1]),
        ]

    for g in range(2):
        for c in here(g):
            c.start()
    p.greet([{"sp": (p.me + k) % n} for k in range(1, n)] + [p.to_core, p.to_pair])

    ones = jnp.ones((8, 2 * bq), jnp.bfloat16)
    pieces = [(i, s) for i in range(kvh) for s in range(strips)]

    def block(st, g, iq, r, key0, bk, diagonal):
        rows, span = pl.ds(pl.multiple_of(iq * bq, bq), bq), pl.ds(pl.multiple_of(key0, bq), bk)
        scores = [
            _dot(kv_s[r, 0, g, i, span, :], q_s[i * strips + s, g, :, rows, :].reshape(wide, HEAD), 1, 1) for i, s in pieces
        ]
        weights, keeps = [], []
        if diagonal:
            ok = lax.rem(lax.broadcasted_iota(jnp.int32, (bk, wide), 1), bq) >= lax.broadcasted_iota(jnp.int32, (bk, wide), 0)
        for (i, s), x in zip(pieces, scores):
            cols = slice(s * wide, (s + 1) * wide)
            if diagonal:
                x = jnp.where(ok, x, HIDDEN)
                top = x.max(axis=0, keepdims=True)
                keeps.append(None)
            else:
                old = top_s[st, i : i + 1, cols]
                top = jnp.maximum(old, x.max(axis=0, keepdims=True))
                keeps.append(jnp.exp2((old - top) * e))
            top_s[st, i : i + 1, cols] = top
            weights.append(jnp.exp2((x - top) * e).astype(jnp.bfloat16))
        for (i, s), w, keep in zip(pieces, weights, keeps):
            cols = slice(s * wide, (s + 1) * wide)
            values = jnp.concatenate([kv_s[r, 1, g, i, span, :].T, ones[:, :bk]], axis=0)
            new = _dot(values, w, 1, 0)
            mix_s[st, i, :, cols] = new if keep is None else mix_s[st, i, :, cols] * keep + new

    phases = 8

    def phase(ph, _):
        g = ph % 2
        kk = ph // 2
        r = jnp.where(kk == 1, n - 1, jnp.where(kk == 0, 0, kk - 1))

        for k in range(len(events)):
            @pl.when(ph == k)
            def _(k=k):
                for f, a in events[k]:
                    f(*a)

        @pl.when(ph < 2)
        def _():
            for c in here(g):
                c.wait()

            def step(iq, _):
                st = g * steps + iq
                block(st, g, iq, 0, iq * bq, bq, True)
                lax.fori_loop(0, iq, lambda b, _: block(st, g, iq, 0, b * bq, bq, False), None)

            lax.fori_loop(0, steps, step, None)

        @pl.when((ph >= 2) & (p.me >= r))
        def _():
            keys(r, g).wait_recv()

            def step(iq, _):
                st = g * steps + iq
                lax.fori_loop(0, tokens // (2 * bq), lambda b, _: block(st, g, iq, r, b * 2 * bq, 2 * bq, False), None)

            lax.fori_loop(0, steps, step, None)

    E = [[] for _ in range(phases)]
    E[0] = [(go_own, (0,)), (send_keys, ((0, 0), (0, 1), (1, 0), (1, 1), (1, 2))), (go_own, (1,))]
    E[1] = [(go_first, (0,))]
    E[2] = [(go_second, (0,)), (go_own, (2,)), (pass_on, ())]
    E[3] = [(go_first, (1,)), (send_keys, ((0, 3),)), (go_own, (3,))]
    E[4] = [(send_keys, ((1, 4),)), (go_second, (1,)), (go_first, (2,)), (go_third, (0,))]
    E[5] = [(send_keys, ((0, 2),)), (go_second, (2,)), (go_first, (3,))]
    E[6] = [(go_third, (1,)), (go_second, (3,))]
    E[7] = [(go_third, (2,))]
    for t in range(8):
        E[t].append((keep_own, (t,)))
    events = E
    lax.fori_loop(0, phases, phase, None)

    def result(g, iq):
        rows, cols = pl.ds(pl.multiple_of(iq * bq, bq), bq), pl.ds(pl.multiple_of(p.core * width, 128), width)
        return stage_s.at[(g * steps + iq) % 2], seen_ref.at[rows, cols]

    def swapped(iq):
        return _remote(*result(1, iq), (rsend, rrecv), iq, p.to_core)

    def stored(iq):
        return pltpu.make_async_copy(*result(0, iq), ssem.at[iq])

    def close(g, iq):
        st, slot = g * steps + iq, (g * steps + iq) % 2
        for i in range(kvh):
            for h in range(2 * strips):
                cols = slice(h * bq, (h + 1) * bq)
                u = mix_s[st, i, :HEAD, cols] * (1 / mix_s[st, i, HEAD : HEAD + 1, cols])
                at = (i * 2 * strips + h) * HEAD
                stage_s[slot, :, at : at + HEAD] = u.T.astype(jnp.bfloat16)

    def close_other(iq, _):
        @pl.when(iq >= 2)
        def _():
            swapped(iq - 2).wait_send()

        close(1, iq)
        swapped(iq).start()

    def close_own(iq, _):
        @pl.when(iq >= 2)
        def _():
            stored(iq - 2).wait()

        close(0, iq)
        stored(iq).start()

    lax.fori_loop(0, steps, close_other, None)
    for iq in (steps - 2, steps - 1):
        swapped(iq).wait_send()
    lax.fori_loop(0, steps, close_own, None)
    go_third(3)
    keep_own(8)
    for iq in (steps - 2, steps - 1):
        stored(iq).wait()
    rows = lambda iq: seen_ref.at[pl.ds(iq * bq, bq), pl.ds(pl.multiple_of((1 - p.core) * width, 128), width)]
    for iq in range(steps):
        _remote(stage_s.at[0], rows(iq), (rsend, rrecv), iq, p.to_core).wait_recv()
    for m in range(cut):
        finish(m)
    for g in range(2):
        for who, copy in key_sends(g):
            pl.when(who)(lambda: keys(*copy).wait_send())
    keep_own(9)


def attend(n, kvq, wo):
    chunks, _, kvh, tokens, _ = kvq.shape
    part, width = wo.shape
    q = chunks - 2
    bq = tokens // 4
    steps = 4
    cut = 4
    unique = part * 13 // 32 // 32 * 32
    cols = (q // kvh) * 2 * bq
    anywhere = pl.BlockSpec(memory_space=pl.ANY)
    scores = 2 * 2 * q * tokens * tokens * n
    return pl.pallas_call(
        functools.partial(_attend, n, bq, cut, unique, HEAD**-0.5 * LOG2E),
        out_shape=[jax.ShapeDtypeStruct((tokens, width), jnp.bfloat16), jax.ShapeDtypeStruct((n * part, width), jnp.bfloat16)],
        in_specs=[anywhere, anywhere],
        out_specs=[anywhere, anywhere],
        scratch_shapes=[
            pltpu.VMEM((q, 2, 2, tokens, HEAD), jnp.bfloat16),
            pltpu.VMEM((n, 2, 2, kvh, tokens, HEAD), jnp.bfloat16),
            pltpu.VMEM((2 * steps, kvh, cols), jnp.float32),
            pltpu.VMEM((2 * steps, kvh, HEAD + 8, cols), jnp.float32),
            pltpu.VMEM((2, bq, q * CHUNK), jnp.bfloat16),
            pltpu.VMEM((2, part // 8, width), jnp.bfloat16),
            pltpu.SemaphoreType.DMA((cut, KINDS)),
            pltpu.SemaphoreType.DMA((cut, KINDS)),
            pltpu.SemaphoreType.DMA((n, 2)),
            pltpu.SemaphoreType.DMA((n, 2)),
            pltpu.SemaphoreType.DMA((steps,)),
            pltpu.SemaphoreType.DMA((steps,)),
            pltpu.SemaphoreType.DMA((2, 2)),
            pltpu.SemaphoreType.DMA((steps,)),
            pltpu.SemaphoreType.DMA((2, 2)),
        ],
        compiler_params=pltpu.CompilerParams(collective_id=1, has_side_effects=True, vmem_limit_bytes=62 * 2**20),
        cost_estimate=pl.CostEstimate(flops=4 * HEAD * scores // 4, transcendentals=scores // 4, bytes_accessed=2**26),
        name="attend",
    )(kvq, wo)


def solution(mesh):
    n = mesh.shape["sp"]

    def step(x, gain, wq, wk, wv, wo):
        tokens = x.shape[0]
        place = lax.axis_index("sp") * tokens + jnp.arange(tokens)
        half = HEAD // 2
        angle = place.astype(jnp.float32)[:, None] * THETA ** (-jnp.arange(half, dtype=jnp.float32) / half)
        cos, sin = jnp.cos(angle), jnp.sin(angle)
        kvq = project(n, x, gain, wk, wv, wq, cos, sin)
        seen, wo = attend(n, kvq, wo)
        y = jnp.dot(seen, wo, preferred_element_type=jnp.float32)
        return (x.astype(jnp.float32) + y).astype(jnp.bfloat16)

    tokens, whole = P(("dp", "sp"), None), P("sp", None)
    return jax.shard_map(
        step,
        mesh=mesh,
        in_specs=(tokens, P(None), whole, whole, whole, whole),
        out_specs=tokens,
        check_vma=False,
    )
```

```python
import functools

import jax
import jax.numpy as jnp
from jax import lax
from jax.experimental import pallas as pl
from jax.experimental.pallas import tpu as pltpu
from jax.sharding import PartitionSpec as P

NEG = -1e30
HIDDEN = 2 * NEG
LOG2E = 1.4426950408889634
HEAD = 128
THETA = 10000
CHUNK = 2 * HEAD
AHEAD = 2
MESH = pl.DeviceIdType.MESH


def _dot(a, b, ca, cb):
    return lax.dot_general(a, b, (((ca,), (cb,)), ((), ())), preferred_element_type=jnp.float32)


def _when(cond, f):
    if isinstance(cond, bool):
        if cond:
            f()
    else:
        pl.when(cond)(f)


def _scores(strips, ok, e, load_top, keep_top, load_mix, keep_mix):
    scores = [_dot(k, q, 1, 1) for _, k, _, q in strips]
    weights, keeps = [], []
    for (name, _, _, _), x in zip(strips, scores):
        if ok is None:
            old = load_top(name)
            top = jnp.maximum(old, x.max(axis=0, keepdims=True))
            keeps.append(jnp.exp2((old - top) * e))
        else:
            x = jnp.where(ok, x, HIDDEN)
            top = x.max(axis=0, keepdims=True)
            keeps.append(None)
        keep_top(name, top)
        weights.append(jnp.exp2((x - top) * e).astype(jnp.bfloat16))
    for (name, _, v, _), w, keep in zip(strips, weights, keeps):
        new = _dot(jnp.concatenate([v.T, jnp.ones((8, v.shape[0]), jnp.bfloat16)], axis=0), w, 1, 0)
        keep_mix(name, new if keep is None else load_mix(name) * keep + new)


class Place:
    def __init__(self, n):
        self.n = n
        self.me = lax.axis_index("sp")
        dp = lax.axis_index("dp")
        self.core, self.half = dp % 2, (dp // 2) % 2
        self.right, self.left, self.far = ((self.me + k) % n for k in (1, n - 1, 2))
        self.to_right, self.to_left = {"sp": self.right}, {"sp": self.left}
        self.to_core = {"dp": dp + 1 - 2 * self.core}
        self.to_pair = {"dp": dp + 2 - 4 * self.half}

    def greet(self, others):
        barrier = pltpu.get_barrier_semaphore()
        for other in others:
            pl.semaphore_signal(barrier, inc=1, device_id=other, device_id_type=MESH)
        pl.semaphore_wait(barrier, len(others))


def _remote(src, dst, sems, at, device):
    send, recv = sems
    return pltpu.make_async_remote_copy(
        src_ref=src, dst_ref=dst, send_sem=send.at[at], recv_sem=recv.at[at], device_id=device, device_id_type=MESH
    )


FROM_LEFT, FROM_RIGHT, ON_RIGHT, ON_LEFT, PAIR_L, PAIR_R, PAIR_F = range(7)


def _project(n, unique, rows, bq, e, x_ref, gain_ref, wk_ref, wv_ref, wq_ref, cos_ref, sin_ref, out_ref, far_ref, mix_ref, top_ref, a_s, w_s,
             stage_s, cos_s, sin_s, gain_s, mix_s, top_s, send, recv, local, xsend, xrecv, xlocal, osem, ksend, krecv, msem):
    p = Place(n)
    chunks, part = w_s.shape[0], wq_ref.shape[0]
    tokens = x_ref.shape[0]
    sems = (send, recv)
    reach = part - unique
    mid = reach // 32 * 16
    off_reach = p.half * unique
    off_mine = p.half * (part - unique)
    off_theirs = (1 - p.half) * (part - unique)
    unit = 16

    def at(j, owner, off, size):
        return w_s.at[j, pl.ds(pl.multiple_of(owner * part + off, unit), size), :]

    def hop(j, kind, owner, off, size, device):
        piece = at(j, owner, off, size)
        return _remote(piece, piece, sems, (j, kind), device)

    def source(j, rows):
        w, first = (wk_ref, 0) if isinstance(j, int) and j == 0 else (wv_ref, 0) if isinstance(j, int) and j == 1 else (wq_ref, jnp.maximum(j - 2, 0))
        return w.at[rows, pl.ds(pl.multiple_of(p.core * (w.shape[1] // 2) + first * CHUNK, HEAD), CHUNK)]

    def own(j):
        src = source(j, pl.ds(pl.multiple_of(off_reach, unit), reach))
        dst = at(j, p.me, off_reach, reach)
        return [
            _remote(src, dst, sems, (j, FROM_LEFT), p.to_right),
            _remote(src, dst, sems, (j, FROM_RIGHT), p.to_left),
        ]

    def kept(j):
        return pltpu.make_async_copy(source(j, pl.ds(0, part)), at(j, p.me, 0, part), local.at[j])

    def from_left(j):
        return hop(j, FROM_LEFT, p.left, off_reach, reach, p.to_right)

    def from_right(j):
        return hop(j, FROM_RIGHT, p.right, off_reach, reach, p.to_left)

    def passed(j):
        return [
            hop(j, ON_RIGHT, p.left, off_reach, mid, p.to_right),
            hop(j, PAIR_L, p.left, off_mine, unique, p.to_pair),
            hop(j, ON_LEFT, p.right, off_reach + mid, reach - mid, p.to_left),
            hop(j, PAIR_R, p.right, off_mine, unique, p.to_pair),
        ]

    def last(j):
        return hop(j, PAIR_F, p.far, off_mine, unique, p.to_pair)

    swap = tokens // 4

    def x_local(t):
        r = pl.ds(t * swap, swap)
        return pltpu.make_async_copy(x_ref.at[r], a_s.at[0, r], xlocal.at[t])

    def x_swap(t):
        r = pl.ds(t * swap, swap)
        return _remote(x_ref.at[r], a_s.at[1, r], (xsend, xrecv), t, p.to_core)

    for t in range(4):
        x_local(t).start()
    p.greet([p.to_right, p.to_left, p.to_core, p.to_pair])
    for j in range(min(AHEAD, chunks)):
        for c in own(j):
            c.start()
        if j == 0:
            for t in range(4):
                x_swap(t).start()

    def keep(j, _):
        kept(j).start()

    keep(0, None)
    keep(1, None)
    lax.fori_loop(2, chunks, keep, None)

    cos_s[...] = jnp.concatenate([cos_ref[...], cos_ref[...]], axis=1)
    sin_s[...] = jnp.concatenate([-sin_ref[...], sin_ref[...]], axis=1)
    for i in range(gain_ref.shape[0]):
        gain_s[:, i * HEAD : (i + 1) * HEAD] = gain_ref[i : i + 1, :].astype(jnp.float32)

    def normalize(g, first, count):
        def body(b, _):
            r = pl.ds(pl.multiple_of(b * 32, 32), 32)
            wide = a_s[g, r, :].astype(jnp.float32)
            scale = lax.rsqrt(jnp.mean(wide * wide, -1, keepdims=True) + 1e-6)
            a_s[g, r, :] = (a_s[g, r, :].astype(jnp.float32) * scale * gain_s[...]).astype(jnp.bfloat16)

        lax.fori_loop(first // 32, (first + count) // 32, body, None)

    def prepare(g):
        for t in range(4):
            if g == 0:
                x_local(t).wait()
            else:
                x_swap(t).wait_recv()
            normalize(g, t * swap, swap)

    def place(j):
        return jnp.where(j < 2, j, 2 + j % 2)

    def compute(j):
        slot = place(j)
        plain = j == 1

        def body(b, _):
            g, m = b // (tokens // rows), b % (tokens // rows)
            r = pl.ds(pl.multiple_of(m * rows, rows), rows)
            t = _dot(a_s[g, r, :], w_s[j], 1, 0).astype(jnp.bfloat16)
            cos, sin = cos_s[r, :], sin_s[r, :]
            for h in range(2):
                u = t[:, h * HEAD : (h + 1) * HEAD].astype(jnp.float32)
                v = u * cos + pltpu.roll(u, HEAD // 2, 1) * sin
                stage_s[slot, g, h, r, :] = jnp.where(plain, u, v).astype(jnp.bfloat16)

        lax.fori_loop(0, 2 * (tokens // rows), body, None)

    def out(j):
        return pltpu.make_async_copy(stage_s.at[place(j)], out_ref.at[j], osem.at[place(j)])

    steps, kvh, wide = tokens // bq, stage_s.shape[2], 2 * bq
    strips = (chunks - 2) // kvh

    def diagonal(j):
        slot, i = 2 + j % 2, (j - 2) // strips
        ok = lax.rem(lax.broadcasted_iota(jnp.int32, (bq, wide), 1), bq) >= lax.broadcasted_iota(jnp.int32, (bq, wide), 0)

        def keep_top(st, top):
            top_s[j % 2, st : st + 1, :] = top

        def keep_mix(st, mix):
            mix_s[j % 2, st] = mix

        for back in range(steps):
            items = []
            for g in range(2):
                for iq in range(back, steps):
                    span, mine = slice((iq - back) * bq, (iq - back + 1) * bq), slice(iq * bq, (iq + 1) * bq)
                    items.append((g * steps + iq, stage_s[0, g, i, span, :], stage_s[1, g, i, span, :], stage_s[slot, g, :, mine, :].reshape(wide, HEAD)))
            _scores(items, ok if back == 0 else None, e, lambda st: top_s[j % 2, st : st + 1, :], keep_top, lambda st: mix_s[j % 2, st], keep_mix)

    def state(j):
        i, cols = (j - 2) // strips, pl.ds(pl.multiple_of((j - 2) % strips * wide, 128), wide)
        return [
            pltpu.make_async_copy(mix_s.at[j % 2], mix_ref.at[:, i, :, cols], msem.at[0, j % 2]),
            pltpu.make_async_copy(top_s.at[j % 2], top_ref.at[i, :, cols], msem.at[1, j % 2]),
        ]

    near, last_one = (p.me < n - 1, 1, p.to_right), (p.me == 0, n - 1, p.to_left)

    def keys(route, piece=None):
        _, r, device = route
        src, dst = out_ref.at[0:2, 0], far_ref.at[r]
        if piece is not None:
            src, dst = (a.at[piece // kvh, piece % kvh] for a in (src, dst))
        return pltpu.make_async_remote_copy(
            src_ref=src, dst_ref=dst, send_sem=ksend.at[r], recv_sem=krecv.at[r], device_id=device, device_id_type=MESH
        )

    begin = max(4, chunks - 1)

    def turn(j, _):
        @pl.when(j < chunks)
        def _():
            from_left(j).wait_recv()
            go = passed(j)
            go[0].start()
            go[1].start()
            from_right(j).wait_recv()
            go[2].start()
            go[3].start()

        @pl.when(j + AHEAD < chunks)
        def _():
            for c in own(j + AHEAD):
                c.start()

        @pl.when(j == begin)
        def _():
            out(0).wait()
            out(1).wait()

        for k in range(2):
            @pl.when(j == begin + k)
            def _(k=k):
                for route in (near, last_one):
                    for piece in range(k * kvh, (k + 1) * kvh):
                        pl.when(route[0])(lambda: keys(route, piece).start())

        for g in range(2):
            pl.when(j == g)(lambda: prepare(g))

        def through():
            i = j - 1
            hop(i, ON_RIGHT, p.far, off_reach, mid, p.to_right).wait_recv()
            hop(i, ON_LEFT, p.far, off_reach + mid, reach - mid, p.to_left).wait_recv()
            last(i).start()

        pl.when((j == 1) | (j == chunks))(through)

        @pl.when(j >= 2)
        def _():
            i = j - 2
            kept(i).wait()
            hop(i, PAIR_L, p.left, off_theirs, unique, p.to_pair).wait_recv()
            hop(i, PAIR_R, p.right, off_theirs, unique, p.to_pair).wait_recv()
            hop(i, PAIR_F, p.far, off_theirs, unique, p.to_pair).wait_recv()

            @pl.when(i >= 4)
            def _():
                out(i - 2).wait()

            compute(i)
            out(i).start()
            pl.when(j < chunks)(through)

            @pl.when(i >= 4)
            def _():
                for c in state(i - 2):
                    c.wait()

            @pl.when(i >= 2)
            def _():
                diagonal(i)
                for c in state(i):
                    c.start()

    lax.fori_loop(0, chunks + 2, turn, None)

    for j in (chunks - 2, chunks - 1):
        for c in [out(j), *state(j)]:
            c.wait()
    pl.when(p.me >= 1)(lambda: keys(near).wait_recv())
    pl.when(p.me == n - 1)(lambda: keys(last_one).wait_recv())
    for route in (near, last_one):
        pl.when(route[0])(lambda: keys(route).wait_send())
    for t in range(4):
        x_swap(t).wait_send()

    def drain(j, _):
        for c in [*own(j), *passed(j), last(j)]:
            c.wait_send()

    lax.fori_loop(0, chunks, drain, None)


def project(n, x, gain, wk, wv, wq, cos, sin):
    tokens, width = x.shape
    part = wq.shape[0]
    chunks = (wk.shape[1] + wv.shape[1] + wq.shape[1]) // (2 * CHUNK)
    unique = part * 10 // 32 // 16 * 16
    rows = min(512, tokens)
    bq = tokens // 4
    kvh = wk.shape[1] // CHUNK
    cols = (chunks - 2) // kvh * 2 * bq
    steps = 8
    anywhere, vmem = pl.BlockSpec(memory_space=pl.ANY), pl.BlockSpec(memory_space=pltpu.VMEM)
    return pl.pallas_call(
        functools.partial(_project, n, unique, rows, bq, HEAD**-0.5 * LOG2E),
        out_shape=[
            jax.ShapeDtypeStruct((chunks, 2, 2, tokens, HEAD), jnp.bfloat16),
            jax.ShapeDtypeStruct((n, 2, kvh, tokens, HEAD), jnp.bfloat16),
            jax.ShapeDtypeStruct((steps, kvh, HEAD + 8, cols), jnp.float32),
            jax.ShapeDtypeStruct((kvh, steps, cols), jnp.float32),
        ],
        in_specs=[anywhere, vmem, anywhere, anywhere, anywhere, vmem, vmem],
        out_specs=[anywhere] * 4,
        scratch_shapes=[
            pltpu.VMEM((2, tokens, width), jnp.bfloat16),
            pltpu.VMEM((chunks, width, CHUNK), jnp.bfloat16),
            pltpu.VMEM((4, 2, 2, tokens, HEAD), jnp.bfloat16),
            pltpu.VMEM((tokens, HEAD), jnp.float32),
            pltpu.VMEM((tokens, HEAD), jnp.float32),
            pltpu.VMEM((1, width), jnp.float32),
            pltpu.VMEM((2, steps, HEAD + 8, 2 * bq), jnp.float32),
            pltpu.VMEM((2, steps, 2 * bq), jnp.float32),
            pltpu.SemaphoreType.DMA((chunks, 7)),
            pltpu.SemaphoreType.DMA((chunks, 7)),
            pltpu.SemaphoreType.DMA((chunks,)),
            pltpu.SemaphoreType.DMA((4,)),
            pltpu.SemaphoreType.DMA((4,)),
            pltpu.SemaphoreType.DMA((4,)),
            pltpu.SemaphoreType.DMA((4,)),
            pltpu.SemaphoreType.DMA((n,)),
            pltpu.SemaphoreType.DMA((n,)),
            pltpu.SemaphoreType.DMA((2, 2)),
        ],
        compiler_params=pltpu.CompilerParams(collective_id=0, has_side_effects=True, vmem_limit_bytes=60 * 2**20),
        cost_estimate=pl.CostEstimate(flops=4 * tokens * width * chunks * CHUNK, transcendentals=0, bytes_accessed=2**26),
        name="project",
    )(x, gain.reshape(-1, HEAD), wk, wv, wq, cos, sin)


A_LEFT, A_RIGHT, F_LEFT, F_RIGHT, Y_L, Y_R, Y_F, D_L, D_R, D_F, E_L, E_R, E_F = range(13)
KINDS = 13


def _attend(n, bq, cut, unique, e, kvq_ref, far_ref, mix_ref, top_ref, wo_ref, seen_ref, all_ref, q_s, kv_s, top_s, mix_s, stage_s, wo_s, send, recv, ksend, krecv, rsend, rrecv, lsem, ssem,
            wsem, msem):
    p = Place(n)
    part = wo_ref.shape[0]
    qchunks, tokens = q_s.shape[0], q_s.shape[3]
    kvh = kv_s.shape[3]
    strips = qchunks // kvh
    wide = 2 * bq
    steps = tokens // bq
    width = qchunks * CHUNK
    cw = width // cut
    reach = part - unique
    off, mid = p.half * unique, reach // 2
    off_mine, other = p.half * reach, (1 - p.half) * reach
    sems = (send, recv)

    def block_of(owner, o, size, core, m):
        return all_ref.at[pl.ds(pl.multiple_of(owner * part + o, 16), size), pl.ds(pl.multiple_of(core * width + m * cw, 128), cw)]

    def hop(m, kind, owner, o, size, device, core=None):
        piece = block_of(owner, o, size, p.core if core is None else core, m)
        return _remote(piece, piece, sems, (m, kind), device)

    def own(m):
        src = wo_ref.at[pl.ds(pl.multiple_of(off, 16), reach), pl.ds(pl.multiple_of(p.core * width + m * cw, 128), cw)]
        dst = block_of(p.me, off, reach, p.core, m)
        return [_remote(src, dst, sems, (m, A_LEFT), p.to_right), _remote(src, dst, sems, (m, A_RIGHT), p.to_left)]

    def first(m):
        return [
            hop(m, F_LEFT, p.left, off, mid, p.to_right),
            hop(m, Y_L, p.left, off_mine, unique, p.to_pair),
            hop(m, D_L, p.left, off, reach, p.to_core),
            hop(m, F_RIGHT, p.right, off + mid, reach - mid, p.to_left),
            hop(m, Y_R, p.right, off_mine, unique, p.to_pair),
            hop(m, D_R, p.right, off, reach, p.to_core),
        ]

    def second(m):
        return [hop(m, Y_F, p.far, off_mine, unique, p.to_pair), hop(m, D_F, p.far, off, reach, p.to_core)]

    def third(m):
        return [
            hop(m, E_L, p.left, other, unique, p.to_core),
            hop(m, E_R, p.right, other, unique, p.to_core),
            hop(m, E_F, p.far, other, unique, p.to_core),
        ]

    def go_own(m):
        for c in own(m):
            c.start()

    def go_first(m):
        hop(m, A_LEFT, p.left, off, reach, p.to_right).wait_recv()
        go = first(m)
        for c in go[:3]:
            c.start()
        hop(m, A_RIGHT, p.right, off, reach, p.to_left).wait_recv()
        for c in go[3:]:
            c.start()

    def go_second(m):
        hop(m, F_LEFT, p.far, off, mid, p.to_right).wait_recv()
        hop(m, F_RIGHT, p.far, off + mid, reach - mid, p.to_left).wait_recv()
        for c in second(m):
            c.start()

    def go_third(m):
        got = [hop(m, Y_L, p.left, other, unique, p.to_pair), hop(m, Y_R, p.right, other, unique, p.to_pair), hop(m, Y_F, p.far, other, unique, p.to_pair)]
        for c, d in zip(got, third(m)):
            c.wait_recv()
            d.start()

    def finish(m):
        core = 1 - p.core
        for kinds, o, size in (((D_L, D_R, D_F), off, reach), ((E_L, E_R, E_F), other, unique)):
            for kind, owner in zip(kinds, (p.left, p.right, p.far)):
                hop(m, kind, owner, o, size, p.to_core, core).wait_recv()
        for c in [*own(m), *first(m), *second(m), *third(m)]:
            c.wait_send()

    def keys(r, g, source=None, device=None, kind=None, piece=None):
        src = kvq_ref.at[0:2, g] if source is None else far_ref.at[source] if g == 0 else kv_s.at[source, :, g]
        dst = kv_s.at[r, :, g]
        if piece is not None:
            src, dst = (a.at[piece // kvh, piece % kvh] for a in (src, dst))
        return pltpu.make_async_remote_copy(
            src_ref=src, dst_ref=dst, send_sem=ksend.at[r if kind is None else kind, g], recv_sem=krecv.at[r, g],
            device_id=p.to_right if device is None else device, device_id_type=MESH,
        )

    key_sends = [
        (p.me < n - 1, (1, 1, None, p.to_right)),
        (p.me == 0, (n - 1, 1, None, p.to_left)),
        (p.me == 1, (1, 1, None, p.to_left, 2)),
        (p.me == 2, (2, 0, 1, p.to_right, 2)),
        (p.me == n - 1, (2, 0, n - 1, p.to_left, 2)),
        (p.me == 0, (2, 1, 1, p.to_left, 2)),
        (p.me == n - 1, (2, 1, n - 1, p.to_left, 2)),
    ]
    NEAR, LAST, BACK, ON_0, ON_LAST_0, ON_1, ON_LAST_1 = range(7)

    def send_keys(at):
        who, copy = key_sends[at]

        @pl.when(who)
        def _():
            for piece in range(2 * kvh):
                keys(*copy, *[None] * (5 - len(copy)), piece).start()

    def take_keys(who, r, g):
        pl.when(p.me == who)(lambda: keys(r, g).wait_recv())

    def brought(r):
        return pltpu.make_async_copy(far_ref.at[r], kv_s.at[r, :, 0], lsem.at[r, 1])

    def state(st):
        return pltpu.make_async_copy(mix_ref.at[st], mix_s.at[st], msem.at[st])

    tops = pltpu.make_async_copy(top_ref, top_s, lsem.at[2, 0])

    strip = part // 8

    def take(t):
        return pltpu.make_async_copy(wo_ref.at[pl.ds(t * strip, strip)], wo_s.at[t % 2], wsem.at[0, t % 2])

    def put(t):
        return pltpu.make_async_copy(
            wo_s.at[t % 2], all_ref.at[pl.ds(pl.multiple_of(p.me * part + t * strip, 16), strip)], wsem.at[1, t % 2]
        )

    def keep_own(t):
        if t >= 2:
            put(t - 2).wait()
        if t < 8:
            take(t).start()
        if 1 <= t <= 8:
            take(t - 1).wait()
            put(t - 1).start()

    def here(g):
        return pltpu.make_async_copy(kvq_ref.at[2:, g], q_s.at[:, g], lsem.at[g, 0])

    here(0).start()
    pl.when(p.me >= 1)(lambda: brought(1).start())
    tops.start()
    state(0).start()
    here(1).start()
    for st in range(1, 2 * steps):
        state(st).start()
    pl.when(p.me == n - 1)(lambda: brought(n - 1).start())
    p.greet([{"sp": (p.me + k) % n} for k in range(1, n)] + [p.to_core, p.to_pair])

    pieces = [(i, s) for i in range(kvh) for s in range(strips)]

    def block(st, g, iq, r, key0, bk):
        rows, span = pl.ds(pl.multiple_of(iq * bq, bq), bq), pl.ds(pl.multiple_of(key0, bq), bk)
        cols = lambda s: slice(s * wide, (s + 1) * wide)

        def keep_top(at, top):
            top_s[at[0], pl.ds(st, 1), cols(at[1])] = top

        def keep_mix(at, mix):
            mix_s[st, at[0], :, cols(at[1])] = mix

        items = [
            ((i, s), kv_s[r, 0, g, i, span, :], kv_s[r, 1, g, i, span, :], q_s[i * strips + s, g, :, rows, :].reshape(wide, HEAD)) for i, s in pieces
        ]
        _scores(items, None, e, lambda at: top_s[at[0], pl.ds(st, 1), cols(at[1])], keep_top, lambda at: mix_s[st, at[0], :, cols(at[1])], keep_mix)

    def result(g, iq):
        rows, cols = pl.ds(pl.multiple_of(iq * bq, bq), bq), pl.ds(pl.multiple_of(p.core * width, 128), width)
        return stage_s.at[iq % 2], seen_ref.at[rows, cols]

    def swapped(iq):
        return _remote(*result(1, iq), (rsend, rrecv), iq, p.to_core)

    def stored(iq):
        return pltpu.make_async_copy(*result(0, iq), ssem.at[iq])

    def close(g, iq):
        st, slot = g * steps + iq, iq % 2
        for i in range(kvh):
            for h in range(2 * strips):
                cols = slice(h * bq, (h + 1) * bq)
                u = mix_s[st, i, :HEAD, cols] * (1 / mix_s[st, i, HEAD : HEAD + 1, cols])
                at = (i * 2 * strips + h) * HEAD
                stage_s[slot, :, at : at + HEAD] = u.T.astype(jnp.bfloat16)

    slots = 2 * (n - 1) * steps
    at_slot = {
        0: [(go_own, (0,)), (send_keys, (NEAR,)), (send_keys, (ON_0,)), (send_keys, (ON_LAST_0,)), (send_keys, (LAST,)), (send_keys, (BACK,))],
        1: [(go_own, (1,))],
        5: [(take_keys, (0, 1, 1)), (send_keys, (ON_1,))],
        6: [(take_keys, (n - 1, n - 1, 1)), (send_keys, (ON_LAST_1,))],
    }
    for t in range(8):
        at_slot.setdefault(2 * t + 3, []).append((keep_own, (t,)))

    def tick(t):
        for k, todo in at_slot.items():
            @pl.when(t == k)
            def _(todo=todo):
                for f, a in todo:
                    f(*a)

        def every(first, f, low):
            m = (t - first + 2 * cut) // 2 - cut
            pl.when((t - first == 2 * m) & (m >= low) & (m < cut))(lambda: f(m))

        pl.when(t == 2)(lambda: go_first(0))
        every(9, go_first, 1)
        every(5, go_own, 2)
        every(12, go_second, 0)
        every(15, go_third, 0)

    def slot(t, _):
        ph, iq = t // steps, t % steps
        g, r = ph % 2, 1 + ph // 2
        st = g * steps + iq
        tick(t)

        @pl.when(t < 2 * steps)
        def _():
            pl.when(t == 0)(lambda: here(0).wait())
            pl.when(t == 0)(lambda: tops.wait())
            pl.when(t == steps)(lambda: here(1).wait())
            state(t).wait()

        @pl.when((t < slots) & (p.me >= r))
        def _():
            pl.when(t == 0)(lambda: brought(1).wait())
            pl.when((iq == 0) & (t > 0) & (r < n - 1))(lambda: keys(r, g).wait_recv())
            pl.when(t == slots - 2 * steps)(lambda: brought(n - 1).wait())
            lax.fori_loop(0, tokens // (2 * bq), lambda b, _: block(st, g, iq, r, b * 2 * bq, 2 * bq), None)

        @pl.when(t >= slots)
        def _():
            k = t - slots
            pl.when((k >= 2) & (k < steps + 2))(lambda: swapped(k - 2).wait_send())
            pl.when(k >= steps + 2)(lambda: stored(k - steps - 2).wait())
            close(1 - k // steps, k % steps)
            pl.when(k < steps)(lambda: swapped(k).start())
            pl.when(k >= steps)(lambda: stored(k - steps).start())

    lax.fori_loop(0, slots + 2 * steps, slot, None)
    keep_own(8)
    for iq in (steps - 2, steps - 1):
        stored(iq).wait()
    rows = lambda iq: seen_ref.at[pl.ds(iq * bq, bq), pl.ds(pl.multiple_of((1 - p.core) * width, 128), width)]
    for iq in range(steps):
        _remote(stage_s.at[0], rows(iq), (rsend, rrecv), iq, p.to_core).wait_recv()
    lax.fori_loop(0, cut, lambda m, _: finish(m), None)
    for who, copy in key_sends:
        pl.when(who)(lambda: keys(*copy).wait_send())
    keep_own(9)


def attend(n, kvq, far, mix, top, wo):
    chunks, _, kvh, tokens, _ = kvq.shape
    part, width = wo.shape
    q = chunks - 2
    bq = tokens // 4
    steps = 4
    cut = min(8, q * CHUNK // 256)
    unique = part * 10 // 32 // 32 * 32
    cols = (q // kvh) * 2 * bq
    anywhere = pl.BlockSpec(memory_space=pl.ANY)
    scores = 2 * 2 * q * tokens * tokens * n
    return pl.pallas_call(
        functools.partial(_attend, n, bq, cut, unique, HEAD**-0.5 * LOG2E),
        out_shape=[jax.ShapeDtypeStruct((tokens, width), jnp.bfloat16), jax.ShapeDtypeStruct((n * part, width), jnp.bfloat16)],
        in_specs=[anywhere] * 5,
        out_specs=[anywhere, anywhere],
        scratch_shapes=[
            pltpu.VMEM((q, 2, 2, tokens, HEAD), jnp.bfloat16),
            pltpu.VMEM((n, 2, 2, kvh, tokens, HEAD), jnp.bfloat16),
            pltpu.VMEM((kvh, 2 * steps, cols), jnp.float32),
            pltpu.VMEM((2 * steps, kvh, HEAD + 8, cols), jnp.float32),
            pltpu.VMEM((2, bq, q * CHUNK), jnp.bfloat16),
            pltpu.VMEM((2, part // 8, width), jnp.bfloat16),
            pltpu.SemaphoreType.DMA((cut, KINDS)),
            pltpu.SemaphoreType.DMA((cut, KINDS)),
            pltpu.SemaphoreType.DMA((n, 2)),
            pltpu.SemaphoreType.DMA((n, 2)),
            pltpu.SemaphoreType.DMA((steps,)),
            pltpu.SemaphoreType.DMA((steps,)),
            pltpu.SemaphoreType.DMA((n, 2)),
            pltpu.SemaphoreType.DMA((steps,)),
            pltpu.SemaphoreType.DMA((2, 2)),
            pltpu.SemaphoreType.DMA((2 * steps,)),
        ],
        compiler_params=pltpu.CompilerParams(collective_id=1, has_side_effects=True, vmem_limit_bytes=62 * 2**20),
        cost_estimate=pl.CostEstimate(flops=4 * HEAD * scores // 4, transcendentals=scores // 4, bytes_accessed=2**26),
        name="attend",
    )(kvq, far, mix, top, wo)


def solution(mesh):
    n = mesh.shape["sp"]

    def step(x, gain, wq, wk, wv, wo):
        tokens = x.shape[0]
        place = lax.axis_index("sp") * tokens + jnp.arange(tokens)
        half = HEAD // 2
        angle = place.astype(jnp.float32)[:, None] * THETA ** (-jnp.arange(half, dtype=jnp.float32) / half)
        cos, sin = jnp.cos(angle), jnp.sin(angle)
        kvq, far, mix, top = project(n, x, gain, wk, wv, wq, cos, sin)
        seen, wo = attend(n, kvq, far, mix, top, wo)
        y = jnp.dot(seen, wo, preferred_element_type=jnp.float32)
        return (x.astype(jnp.float32) + y).astype(jnp.bfloat16)

    tokens, whole = P(("dp", "sp"), None), P("sp", None)
    return jax.shard_map(
        step,
        mesh=mesh,
        in_specs=(tokens, P(None), whole, whole, whole, whole),
        out_specs=tokens,
        check_vma=False,
    )
```

```python
import functools

import jax
import jax.numpy as jnp
from jax import lax
from jax.experimental import pallas as pl
from jax.experimental.pallas import tpu as pltpu
from jax.sharding import PartitionSpec as P

NEG = -1e30
HIDDEN = 2 * NEG
LOG2E = 1.4426950408889634
HEAD = 128
THETA = 10000
CHUNK = 2 * HEAD
AHEAD = 2
MESH = pl.DeviceIdType.MESH


def _dot(a, b, ca, cb):
    return lax.dot_general(a, b, (((ca,), (cb,)), ((), ())), preferred_element_type=jnp.float32)


def _when(cond, f):
    if isinstance(cond, bool):
        if cond:
            f()
    else:
        pl.when(cond)(f)


def _scores(strips, ok, e, load_top, keep_top, load_mix, keep_mix):
    scores = [_dot(k, q, 1, 1) for _, k, _, q in strips]
    weights, keeps = [], []
    for (name, _, _, _), x in zip(strips, scores):
        if ok is None:
            old = load_top(name)
            top = jnp.maximum(old, x.max(axis=0, keepdims=True))
            keeps.append(jnp.exp2((old - top) * e))
        else:
            x = jnp.where(ok, x, HIDDEN)
            top = x.max(axis=0, keepdims=True)
            keeps.append(None)
        keep_top(name, top)
        weights.append(jnp.exp2((x - top) * e).astype(jnp.bfloat16))
    for (name, _, v, _), w, keep in zip(strips, weights, keeps):
        new = _dot(jnp.concatenate([v.T, jnp.ones((8, v.shape[0]), jnp.bfloat16)], axis=0), w, 1, 0)
        keep_mix(name, new if keep is None else load_mix(name) * keep + new)


class Place:
    def __init__(self, n):
        self.n = n
        self.me = lax.axis_index("sp")
        dp = lax.axis_index("dp")
        self.core, self.half = dp % 2, (dp // 2) % 2
        self.right, self.left, self.far = ((self.me + k) % n for k in (1, n - 1, 2))
        self.to_right, self.to_left = {"sp": self.right}, {"sp": self.left}
        self.to_core = {"dp": dp + 1 - 2 * self.core}
        self.to_pair = {"dp": dp + 2 - 4 * self.half}

    def greet(self, others):
        barrier = pltpu.get_barrier_semaphore()
        for other in others:
            pl.semaphore_signal(barrier, inc=1, device_id=other, device_id_type=MESH)
        pl.semaphore_wait(barrier, len(others))


def _remote(src, dst, sems, at, device):
    send, recv = sems
    return pltpu.make_async_remote_copy(
        src_ref=src, dst_ref=dst, send_sem=send.at[at], recv_sem=recv.at[at], device_id=device, device_id_type=MESH
    )


FROM_LEFT, FROM_RIGHT, ON_RIGHT, ON_LEFT, PAIR_L, PAIR_R, PAIR_F = range(7)


def _project(n, unique, rows, bq, e, x_ref, gain_ref, wk_ref, wv_ref, wq_ref, cos_ref, sin_ref, out_ref, far_ref, mix_ref, top_ref, a_s, w_s,
             stage_s, cos_s, sin_s, gain_s, mix_s, top_s, send, recv, local, xsend, xrecv, xlocal, osem, ksend, krecv, msem):
    p = Place(n)
    chunks, part = w_s.shape[0], wq_ref.shape[0]
    tokens = x_ref.shape[0]
    sems = (send, recv)
    reach = part - unique
    mid = reach // 32 * 16
    off_reach = p.half * unique
    off_mine = p.half * (part - unique)
    off_theirs = (1 - p.half) * (part - unique)
    unit = 16

    def at(j, owner, off, size):
        return w_s.at[j, pl.ds(pl.multiple_of(owner * part + off, unit), size), :]

    def hop(j, kind, owner, off, size, device):
        piece = at(j, owner, off, size)
        return _remote(piece, piece, sems, (j, kind), device)

    def source(j, rows):
        w, first = (wk_ref, 0) if isinstance(j, int) and j == 0 else (wv_ref, 0) if isinstance(j, int) and j == 1 else (wq_ref, jnp.maximum(j - 2, 0))
        return w.at[rows, pl.ds(pl.multiple_of(p.core * (w.shape[1] // 2) + first * CHUNK, HEAD), CHUNK)]

    def own(j):
        src = source(j, pl.ds(pl.multiple_of(off_reach, unit), reach))
        dst = at(j, p.me, off_reach, reach)
        return [
            _remote(src, dst, sems, (j, FROM_LEFT), p.to_right),
            _remote(src, dst, sems, (j, FROM_RIGHT), p.to_left),
        ]

    def kept(j):
        return pltpu.make_async_copy(source(j, pl.ds(0, part)), at(j, p.me, 0, part), local.at[j])

    def from_left(j):
        return hop(j, FROM_LEFT, p.left, off_reach, reach, p.to_right)

    def from_right(j):
        return hop(j, FROM_RIGHT, p.right, off_reach, reach, p.to_left)

    def passed(j):
        return [
            hop(j, ON_RIGHT, p.left, off_reach, mid, p.to_right),
            hop(j, PAIR_L, p.left, off_mine, unique, p.to_pair),
            hop(j, ON_LEFT, p.right, off_reach + mid, reach - mid, p.to_left),
            hop(j, PAIR_R, p.right, off_mine, unique, p.to_pair),
        ]

    def last(j):
        return hop(j, PAIR_F, p.far, off_mine, unique, p.to_pair)

    swap = tokens // 4

    def x_local(t):
        r = pl.ds(t * swap, swap)
        return pltpu.make_async_copy(x_ref.at[r], a_s.at[0, r], xlocal.at[t])

    def x_swap(t):
        r = pl.ds(t * swap, swap)
        return _remote(x_ref.at[r], a_s.at[1, r], (xsend, xrecv), t, p.to_core)

    for t in range(4):
        x_local(t).start()
    p.greet([p.to_right, p.to_left, p.to_core, p.to_pair])
    for j in range(min(AHEAD, chunks)):
        for c in own(j):
            c.start()
        if j == 0:
            for t in range(4):
                x_swap(t).start()

    def keep(j, _):
        kept(j).start()

    keep(0, None)
    keep(1, None)
    lax.fori_loop(2, chunks, keep, None)

    cos_s[...] = jnp.concatenate([cos_ref[...], cos_ref[...]], axis=1)
    sin_s[...] = jnp.concatenate([-sin_ref[...], sin_ref[...]], axis=1)
    for i in range(gain_ref.shape[0]):
        gain_s[:, i * HEAD : (i + 1) * HEAD] = gain_ref[i : i + 1, :].astype(jnp.float32)

    def normalize(g, first, count):
        def body(b, _):
            r = pl.ds(pl.multiple_of(b * 32, 32), 32)
            wide = a_s[g, r, :].astype(jnp.float32)
            scale = lax.rsqrt(jnp.mean(wide * wide, -1, keepdims=True) + 1e-6)
            a_s[g, r, :] = (a_s[g, r, :].astype(jnp.float32) * scale * gain_s[...]).astype(jnp.bfloat16)

        lax.fori_loop(first // 32, (first + count) // 32, body, None)

    def prepare(g):
        for t in range(4):
            if g == 0:
                x_local(t).wait()
            else:
                x_swap(t).wait_recv()
            normalize(g, t * swap, swap)

    def place(j):
        return jnp.where(j < 2, j, 2 + j % 2)

    def compute(j):
        slot = place(j)
        plain = j == 1

        def body(b, _):
            g, m = b // (tokens // rows), b % (tokens // rows)
            r = pl.ds(pl.multiple_of(m * rows, rows), rows)
            t = _dot(a_s[g, r, :], w_s[j], 1, 0).astype(jnp.bfloat16)
            cos, sin = cos_s[r, :], sin_s[r, :]
            for h in range(2):
                u = t[:, h * HEAD : (h + 1) * HEAD].astype(jnp.float32)
                v = u * cos + pltpu.roll(u, HEAD // 2, 1) * sin
                stage_s[slot, g, h, r, :] = jnp.where(plain, u, v).astype(jnp.bfloat16)

        lax.fori_loop(0, 2 * (tokens // rows), body, None)

    def out(j):
        return pltpu.make_async_copy(stage_s.at[place(j)], out_ref.at[j], osem.at[place(j)])

    steps, kvh, wide = tokens // bq, stage_s.shape[2], 2 * bq
    strips = (chunks - 2) // kvh

    def diagonal(j):
        slot, i = 2 + j % 2, (j - 2) // strips
        ok = lax.rem(lax.broadcasted_iota(jnp.int32, (bq, wide), 1), bq) >= lax.broadcasted_iota(jnp.int32, (bq, wide), 0)

        def keep_top(st, top):
            top_s[j % 2, st : st + 1, :] = top

        def keep_mix(st, mix):
            mix_s[j % 2, st] = mix

        for back in range(steps):
            items = []
            for g in range(2):
                for iq in range(back, steps):
                    span, mine = slice((iq - back) * bq, (iq - back + 1) * bq), slice(iq * bq, (iq + 1) * bq)
                    items.append((g * steps + iq, stage_s[0, g, i, span, :], stage_s[1, g, i, span, :], stage_s[slot, g, :, mine, :].reshape(wide, HEAD)))
            _scores(items, ok if back == 0 else None, e, lambda st: top_s[j % 2, st : st + 1, :], keep_top, lambda st: mix_s[j % 2, st], keep_mix)

    def state(j):
        i, cols = (j - 2) // strips, pl.ds(pl.multiple_of((j - 2) % strips * wide, 128), wide)
        return [
            pltpu.make_async_copy(mix_s.at[j % 2], mix_ref.at[:, i, :, cols], msem.at[0, j % 2]),
            pltpu.make_async_copy(top_s.at[j % 2], top_ref.at[i, :, cols], msem.at[1, j % 2]),
        ]

    near, last_one = (p.me < n - 1, 1, p.to_right), (p.me == 0, n - 1, p.to_left)

    def keys(route, piece=None):
        _, r, device = route
        src, dst = out_ref.at[0:2, 0], far_ref.at[r]
        if piece is not None:
            src, dst = (a.at[piece // kvh, piece % kvh] for a in (src, dst))
        return pltpu.make_async_remote_copy(
            src_ref=src, dst_ref=dst, send_sem=ksend.at[r], recv_sem=krecv.at[r], device_id=device, device_id_type=MESH
        )

    begin = max(4, chunks - 1)

    def turn(j, _):
        @pl.when(j < chunks)
        def _():
            from_left(j).wait_recv()
            go = passed(j)
            go[0].start()
            go[1].start()
            from_right(j).wait_recv()
            go[2].start()
            go[3].start()

        @pl.when(j + AHEAD < chunks)
        def _():
            for c in own(j + AHEAD):
                c.start()

        @pl.when(j == begin)
        def _():
            out(0).wait()
            out(1).wait()

        for k in range(2):
            @pl.when(j == begin + k)
            def _(k=k):
                for route in (near, last_one):
                    for piece in range(k * kvh, (k + 1) * kvh):
                        pl.when(route[0])(lambda: keys(route, piece).start())

        for g in range(2):
            pl.when(j == g)(lambda: prepare(g))

        def through():
            i = j - 1
            hop(i, ON_RIGHT, p.far, off_reach, mid, p.to_right).wait_recv()
            hop(i, ON_LEFT, p.far, off_reach + mid, reach - mid, p.to_left).wait_recv()
            last(i).start()

        pl.when((j == 1) | (j == chunks))(through)

        @pl.when(j >= 2)
        def _():
            i = j - 2
            kept(i).wait()
            hop(i, PAIR_L, p.left, off_theirs, unique, p.to_pair).wait_recv()
            hop(i, PAIR_R, p.right, off_theirs, unique, p.to_pair).wait_recv()
            hop(i, PAIR_F, p.far, off_theirs, unique, p.to_pair).wait_recv()

            @pl.when(i >= 4)
            def _():
                out(i - 2).wait()

            compute(i)
            out(i).start()
            pl.when(j < chunks)(through)

            @pl.when(i >= 4)
            def _():
                for c in state(i - 2):
                    c.wait()

            @pl.when(i >= 2)
            def _():
                diagonal(i)
                for c in state(i):
                    c.start()

    lax.fori_loop(0, chunks + 2, turn, None)

    for j in (chunks - 2, chunks - 1):
        for c in [out(j), *state(j)]:
            c.wait()
    pl.when(p.me >= 1)(lambda: keys(near).wait_recv())
    pl.when(p.me == n - 1)(lambda: keys(last_one).wait_recv())
    for route in (near, last_one):
        pl.when(route[0])(lambda: keys(route).wait_send())
    for t in range(4):
        x_swap(t).wait_send()

    def drain(j, _):
        for c in [*own(j), *passed(j), last(j)]:
            c.wait_send()

    lax.fori_loop(0, chunks, drain, None)


def project(n, x, gain, wk, wv, wq, cos, sin):
    tokens, width = x.shape
    part = wq.shape[0]
    chunks = (wk.shape[1] + wv.shape[1] + wq.shape[1]) // (2 * CHUNK)
    unique = part * 10 // 32 // 16 * 16
    rows = min(1024, tokens)
    bq = tokens // 4
    kvh = wk.shape[1] // CHUNK
    cols = (chunks - 2) // kvh * 2 * bq
    steps = 8
    anywhere, vmem = pl.BlockSpec(memory_space=pl.ANY), pl.BlockSpec(memory_space=pltpu.VMEM)
    return pl.pallas_call(
        functools.partial(_project, n, unique, rows, bq, HEAD**-0.5 * LOG2E),
        out_shape=[
            jax.ShapeDtypeStruct((chunks, 2, 2, tokens, HEAD), jnp.bfloat16),
            jax.ShapeDtypeStruct((n, 2, kvh, tokens, HEAD), jnp.bfloat16),
            jax.ShapeDtypeStruct((steps, kvh, HEAD + 8, cols), jnp.float32),
            jax.ShapeDtypeStruct((kvh, steps, cols), jnp.float32),
        ],
        in_specs=[anywhere, vmem, anywhere, anywhere, anywhere, vmem, vmem],
        out_specs=[anywhere] * 4,
        scratch_shapes=[
            pltpu.VMEM((2, tokens, width), jnp.bfloat16),
            pltpu.VMEM((chunks, width, CHUNK), jnp.bfloat16),
            pltpu.VMEM((4, 2, 2, tokens, HEAD), jnp.bfloat16),
            pltpu.VMEM((tokens, HEAD), jnp.float32),
            pltpu.VMEM((tokens, HEAD), jnp.float32),
            pltpu.VMEM((1, width), jnp.float32),
            pltpu.VMEM((2, steps, HEAD + 8, 2 * bq), jnp.float32),
            pltpu.VMEM((2, steps, 2 * bq), jnp.float32),
            pltpu.SemaphoreType.DMA((chunks, 7)),
            pltpu.SemaphoreType.DMA((chunks, 7)),
            pltpu.SemaphoreType.DMA((chunks,)),
            pltpu.SemaphoreType.DMA((4,)),
            pltpu.SemaphoreType.DMA((4,)),
            pltpu.SemaphoreType.DMA((4,)),
            pltpu.SemaphoreType.DMA((4,)),
            pltpu.SemaphoreType.DMA((n,)),
            pltpu.SemaphoreType.DMA((n,)),
            pltpu.SemaphoreType.DMA((2, 2)),
        ],
        compiler_params=pltpu.CompilerParams(collective_id=0, has_side_effects=True, vmem_limit_bytes=60 * 2**20),
        cost_estimate=pl.CostEstimate(flops=4 * tokens * width * chunks * CHUNK, transcendentals=0, bytes_accessed=2**26),
        name="project",
    )(x, gain.reshape(-1, HEAD), wk, wv, wq, cos, sin)


A_LEFT, A_RIGHT, F_LEFT, F_RIGHT, Y_L, Y_R, Y_F, D_L, D_R, D_F, E_L, E_R, E_F = range(13)
KINDS = 13


def _attend(n, bq, cut, unique, e, kvq_ref, far_ref, mix_ref, top_ref, wo_ref, seen_ref, all_ref, q_s, kv_s, top_s, mix_s, stage_s, wo_s, send, recv, ksend, krecv, rsend, rrecv, lsem, ssem,
            wsem, msem):
    p = Place(n)
    part = wo_ref.shape[0]
    qchunks, tokens = q_s.shape[0], q_s.shape[3]
    kvh = kv_s.shape[3]
    strips = qchunks // kvh
    wide = 2 * bq
    steps = tokens // bq
    width = qchunks * CHUNK
    cw = width // cut
    reach = part - unique
    off, mid = p.half * unique, reach // 2
    off_mine, other = p.half * reach, (1 - p.half) * reach
    sems = (send, recv)

    def block_of(owner, o, size, core, m):
        return all_ref.at[pl.ds(pl.multiple_of(owner * part + o, 16), size), pl.ds(pl.multiple_of(core * width + m * cw, 128), cw)]

    def hop(m, kind, owner, o, size, device, core=None):
        piece = block_of(owner, o, size, p.core if core is None else core, m)
        return _remote(piece, piece, sems, (m, kind), device)

    def own(m):
        src = wo_ref.at[pl.ds(pl.multiple_of(off, 16), reach), pl.ds(pl.multiple_of(p.core * width + m * cw, 128), cw)]
        dst = block_of(p.me, off, reach, p.core, m)
        return [_remote(src, dst, sems, (m, A_LEFT), p.to_right), _remote(src, dst, sems, (m, A_RIGHT), p.to_left)]

    def first(m):
        return [
            hop(m, F_LEFT, p.left, off, mid, p.to_right),
            hop(m, Y_L, p.left, off_mine, unique, p.to_pair),
            hop(m, D_L, p.left, off, reach, p.to_core),
            hop(m, F_RIGHT, p.right, off + mid, reach - mid, p.to_left),
            hop(m, Y_R, p.right, off_mine, unique, p.to_pair),
            hop(m, D_R, p.right, off, reach, p.to_core),
        ]

    def second(m):
        return [hop(m, Y_F, p.far, off_mine, unique, p.to_pair), hop(m, D_F, p.far, off, reach, p.to_core)]

    def third(m):
        return [
            hop(m, E_L, p.left, other, unique, p.to_core),
            hop(m, E_R, p.right, other, unique, p.to_core),
            hop(m, E_F, p.far, other, unique, p.to_core),
        ]

    def go_own(m):
        for c in own(m):
            c.start()

    def go_first(m):
        hop(m, A_LEFT, p.left, off, reach, p.to_right).wait_recv()
        go = first(m)
        for c in go[:3]:
            c.start()
        hop(m, A_RIGHT, p.right, off, reach, p.to_left).wait_recv()
        for c in go[3:]:
            c.start()

    def go_second(m):
        hop(m, F_LEFT, p.far, off, mid, p.to_right).wait_recv()
        hop(m, F_RIGHT, p.far, off + mid, reach - mid, p.to_left).wait_recv()
        for c in second(m):
            c.start()

    def go_third(m):
        got = [hop(m, Y_L, p.left, other, unique, p.to_pair), hop(m, Y_R, p.right, other, unique, p.to_pair), hop(m, Y_F, p.far, other, unique, p.to_pair)]
        for c, d in zip(got, third(m)):
            c.wait_recv()
            d.start()

    def finish(m):
        core = 1 - p.core
        for kinds, o, size in (((D_L, D_R, D_F), off, reach), ((E_L, E_R, E_F), other, unique)):
            for kind, owner in zip(kinds, (p.left, p.right, p.far)):
                hop(m, kind, owner, o, size, p.to_core, core).wait_recv()
        for c in [*own(m), *first(m), *second(m), *third(m)]:
            c.wait_send()

    def keys(r, g, source=None, device=None, kind=None, piece=None):
        src = kvq_ref.at[0:2, g] if source is None else far_ref.at[source] if g == 0 else kv_s.at[source, :, g]
        dst = kv_s.at[r, :, g]
        if piece is not None:
            src, dst = (a.at[piece // kvh, piece % kvh] for a in (src, dst))
        return pltpu.make_async_remote_copy(
            src_ref=src, dst_ref=dst, send_sem=ksend.at[r if kind is None else kind, g], recv_sem=krecv.at[r, g],
            device_id=p.to_right if device is None else device, device_id_type=MESH,
        )

    key_sends = [
        (p.me < n - 1, (1, 1, None, p.to_right)),
        (p.me == 0, (n - 1, 1, None, p.to_left)),
        (p.me == 1, (1, 1, None, p.to_left, 2)),
        (p.me == 2, (2, 0, 1, p.to_right, 2)),
        (p.me == n - 1, (2, 0, n - 1, p.to_left, 2)),
        (p.me == 0, (2, 1, 1, p.to_left, 2)),
        (p.me == n - 1, (2, 1, n - 1, p.to_left, 2)),
    ]
    NEAR, LAST, BACK, ON_0, ON_LAST_0, ON_1, ON_LAST_1 = range(7)

    def send_keys(at):
        who, copy = key_sends[at]

        @pl.when(who)
        def _():
            for piece in range(2 * kvh):
                keys(*copy, *[None] * (5 - len(copy)), piece).start()

    def take_keys(who, r, g):
        pl.when(p.me == who)(lambda: keys(r, g).wait_recv())

    def brought(r):
        return pltpu.make_async_copy(far_ref.at[r], kv_s.at[r, :, 0], lsem.at[r, 1])

    def state(st):
        return pltpu.make_async_copy(mix_ref.at[st], mix_s.at[st], msem.at[st])

    tops = pltpu.make_async_copy(top_ref, top_s, lsem.at[2, 0])

    strip = part // 8

    def take(t):
        return pltpu.make_async_copy(wo_ref.at[pl.ds(t * strip, strip)], wo_s.at[t % 2], wsem.at[0, t % 2])

    def put(t):
        return pltpu.make_async_copy(
            wo_s.at[t % 2], all_ref.at[pl.ds(pl.multiple_of(p.me * part + t * strip, 16), strip)], wsem.at[1, t % 2]
        )

    def keep_own(t):
        if t >= 2:
            put(t - 2).wait()
        if t < 8:
            take(t).start()
        if 1 <= t <= 8:
            take(t - 1).wait()
            put(t - 1).start()

    def here(g):
        return pltpu.make_async_copy(kvq_ref.at[2:, g], q_s.at[:, g], lsem.at[g, 0])

    here(0).start()
    pl.when(p.me >= 1)(lambda: brought(1).start())
    tops.start()
    state(0).start()
    here(1).start()
    for st in range(1, 2 * steps):
        state(st).start()
    pl.when(p.me == n - 1)(lambda: brought(n - 1).start())
    p.greet([{"sp": (p.me + k) % n} for k in range(1, n)] + [p.to_core, p.to_pair])

    def block(st, g, iq, r, i):
        rows, span = pl.ds(pl.multiple_of(iq * bq, bq), bq), slice(None)
        cols = lambda s: slice(s * wide, (s + 1) * wide)

        def keep_top(at, top):
            top_s[i, pl.ds(st, 1), cols(at)] = top

        def keep_mix(at, mix):
            mix_s[st, i, :, cols(at)] = mix

        items = [
            (s, kv_s[r, 0, g, i, span, :], kv_s[r, 1, g, i, span, :], q_s[i * strips + s, g, :, rows, :].reshape(wide, HEAD)) for s in range(strips)
        ]
        _scores(items, None, e, lambda at: top_s[i, pl.ds(st, 1), cols(at)], keep_top, lambda at: mix_s[st, i, :, cols(at)], keep_mix)

    def result(g, iq):
        rows, cols = pl.ds(pl.multiple_of(iq * bq, bq), bq), pl.ds(pl.multiple_of(p.core * width, 128), width)
        return stage_s.at[iq % 2], seen_ref.at[rows, cols]

    def swapped(iq):
        return _remote(*result(1, iq), (rsend, rrecv), iq, p.to_core)

    def stored(iq):
        return pltpu.make_async_copy(*result(0, iq), ssem.at[iq])

    def close(g, iq):
        st, slot = g * steps + iq, iq % 2
        for i in range(kvh):
            for h in range(2 * strips):
                cols = slice(h * bq, (h + 1) * bq)
                u = mix_s[st, i, :HEAD, cols] * (1 / mix_s[st, i, HEAD : HEAD + 1, cols])
                at = (i * 2 * strips + h) * HEAD
                stage_s[slot, :, at : at + HEAD] = u.T.astype(jnp.bfloat16)

    slots = 2 * (n - 1) * steps
    at_slot = {
        0: [(go_own, (0,)), (send_keys, (NEAR,)), (send_keys, (ON_0,)), (send_keys, (ON_LAST_0,)), (send_keys, (LAST,)), (send_keys, (BACK,))],
        1: [(go_own, (1,))],
        5: [(take_keys, (0, 1, 1)), (send_keys, (ON_1,))],
        6: [(take_keys, (n - 1, n - 1, 1)), (send_keys, (ON_LAST_1,))],
    }
    for t in range(8):
        at_slot.setdefault(2 * t + 3, []).append((keep_own, (t,)))

    def tick(t):
        for k, todo in at_slot.items():
            @pl.when(t == k)
            def _(todo=todo):
                for f, a in todo:
                    f(*a)

        def every(first, f, low):
            m = (t - first + 2 * cut) // 2 - cut
            pl.when((t - first == 2 * m) & (m >= low) & (m < cut))(lambda: f(m))

        pl.when(t == 2)(lambda: go_first(0))
        every(9, go_first, 1)
        every(5, go_own, 2)
        every(12, go_second, 0)
        every(15, go_third, 0)

    def slot(t, _):
        ph, iq = t // steps, t % steps
        g, r = ph % 2, 1 + ph // 2
        st = g * steps + iq
        tick(t)

        @pl.when(t < 2 * steps)
        def _():
            pl.when(t == 0)(lambda: here(0).wait())
            pl.when(t == 0)(lambda: tops.wait())
            pl.when(t == steps)(lambda: here(1).wait())
            state(t).wait()

        @pl.when((t < slots) & (p.me >= r))
        def _():
            pl.when(t == 0)(lambda: brought(1).wait())
            pl.when((iq == 0) & (t > 0) & (r < n - 1))(lambda: keys(r, g).wait_recv())
            pl.when(t == slots - 2 * steps)(lambda: brought(n - 1).wait())
            lax.fori_loop(0, kvh, lambda i, _: block(st, g, iq, r, i), None)

        @pl.when(t >= slots)
        def _():
            k = t - slots
            pl.when((k >= 2) & (k < steps + 2))(lambda: swapped(k - 2).wait_send())
            pl.when(k >= steps + 2)(lambda: stored(k - steps - 2).wait())
            close(1 - k // steps, k % steps)
            pl.when(k < steps)(lambda: swapped(k).start())
            pl.when(k >= steps)(lambda: stored(k - steps).start())

    lax.fori_loop(0, slots + 2 * steps, slot, None)
    keep_own(8)
    for iq in (steps - 2, steps - 1):
        stored(iq).wait()
    rows = lambda iq: seen_ref.at[pl.ds(iq * bq, bq), pl.ds(pl.multiple_of((1 - p.core) * width, 128), width)]
    for iq in range(steps):
        _remote(stage_s.at[0], rows(iq), (rsend, rrecv), iq, p.to_core).wait_recv()
    lax.fori_loop(0, cut, lambda m, _: finish(m), None)
    for who, copy in key_sends:
        pl.when(who)(lambda: keys(*copy).wait_send())
    keep_own(9)


def attend(n, kvq, far, mix, top, wo):
    chunks, _, kvh, tokens, _ = kvq.shape
    part, width = wo.shape
    q = chunks - 2
    bq = tokens // 4
    steps = 4
    cut = min(8, q * CHUNK // 256)
    unique = part * 10 // 32 // 32 * 32
    cols = (q // kvh) * 2 * bq
    anywhere = pl.BlockSpec(memory_space=pl.ANY)
    scores = 2 * 2 * q * tokens * tokens * n
    return pl.pallas_call(
        functools.partial(_attend, n, bq, cut, unique, HEAD**-0.5 * LOG2E),
        out_shape=[jax.ShapeDtypeStruct((tokens, width), jnp.bfloat16), jax.ShapeDtypeStruct((n * part, width), jnp.bfloat16)],
        in_specs=[anywhere] * 5,
        out_specs=[anywhere, anywhere],
        scratch_shapes=[
            pltpu.VMEM((q, 2, 2, tokens, HEAD), jnp.bfloat16),
            pltpu.VMEM((n, 2, 2, kvh, tokens, HEAD), jnp.bfloat16),
            pltpu.VMEM((kvh, 2 * steps, cols), jnp.float32),
            pltpu.VMEM((2 * steps, kvh, HEAD + 8, cols), jnp.float32),
            pltpu.VMEM((2, bq, q * CHUNK), jnp.bfloat16),
            pltpu.VMEM((2, part // 8, width), jnp.bfloat16),
            pltpu.SemaphoreType.DMA((cut, KINDS)),
            pltpu.SemaphoreType.DMA((cut, KINDS)),
            pltpu.SemaphoreType.DMA((n, 2)),
            pltpu.SemaphoreType.DMA((n, 2)),
            pltpu.SemaphoreType.DMA((steps,)),
            pltpu.SemaphoreType.DMA((steps,)),
            pltpu.SemaphoreType.DMA((n, 2)),
            pltpu.SemaphoreType.DMA((steps,)),
            pltpu.SemaphoreType.DMA((2, 2)),
            pltpu.SemaphoreType.DMA((2 * steps,)),
        ],
        compiler_params=pltpu.CompilerParams(collective_id=1, has_side_effects=True, vmem_limit_bytes=62 * 2**20),
        cost_estimate=pl.CostEstimate(flops=4 * HEAD * scores // 4, transcendentals=scores // 4, bytes_accessed=2**26),
        name="attend",
    )(kvq, far, mix, top, wo)


def solution(mesh):
    n = mesh.shape["sp"]

    def step(x, gain, wq, wk, wv, wo):
        tokens = x.shape[0]
        place = lax.axis_index("sp") * tokens + jnp.arange(tokens)
        half = HEAD // 2
        angle = place.astype(jnp.float32)[:, None] * THETA ** (-jnp.arange(half, dtype=jnp.float32) / half)
        cos, sin = jnp.cos(angle), jnp.sin(angle)
        kvq, far, mix, top = project(n, x, gain, wk, wv, wq, cos, sin)
        seen, wo = attend(n, kvq, far, mix, top, wo)
        y = jnp.dot(seen, wo, preferred_element_type=jnp.float32)
        return (x.astype(jnp.float32) + y).astype(jnp.bfloat16)

    tokens, whole = P(("dp", "sp"), None), P("sp", None)
    return jax.shard_map(
        step,
        mesh=mesh,
        in_specs=(tokens, P(None), whole, whole, whole, whole),
        out_specs=tokens,
        check_vma=False,
    )
```
